128 devices in a mesh: var: 16 (over x, y), samp: 8 (over z, core).
Axes of the slice: x: 4, y: 4, z: 4, core: 2. Of those that a mesh axis runs over, the one named last changes fastest.
Arguments:
- dosage: int32 [24576, 8192], P('samp', 'var'), may hold values from 0 to 2, as said below
- phenotype: float32 [24576], P('samp'), may hold values from -6 to 6
- perm_index: int32 [1024, 24576], P('var', 'samp'), may hold values from 0 to 24575, each once within a row
- seg_lengths: int32 [128], replicated, may hold values from 1 to 128, 8192 in all
Outputs:
- zscore: float32 [1024, 8192], P('samp', 'var')
- thresholds: float32 [1024, 128], P('samp')
The draws below stay inside these ranges and needn't reach their ends.
Inputs may be any that keep to these rules, and one draw needn't show every extreme that they name: `dosage`: each entry is an allele count. `perm_index`: each row is a permutation of the 24576 sample numbers. `seg_lengths`: the lengths sum to 8192, one of them equals 128.
All inputs are finite; a program needn't handle non-finite values.
Results may differ from the reference program's by a relative error of at most 0.0039.
Values may be sent and summed in bfloat16 or wider, within the bound.
A program may use at most 64 MiB of HBM per device.

```python
import math
import jax
import jax.numpy as jnp
import numpy as np
from jax import lax

PERMS = 1024
SEGS = 128
SAMPLES = 24576
V = 8192
SEG_MOST = 128


def draw_dosage(key, part):
    rate_key, one_key, two_key = jax.random.split(jax.random.fold_in(key, 17), 3)
    allele_rate = jax.random.randint(rate_key, (1, V), 20, 300)
    cohort_rise = 1000 + 2000 * jnp.arange(SAMPLES, dtype=jnp.int32) // SAMPLES
    level = allele_rate * cohort_rise[:, None] // 1000
    allele_one = jax.random.randint(one_key, (SAMPLES, V), 0, 1000) < level
    allele_two = jax.random.randint(two_key, (SAMPLES, V), 0, 1000) < level
    return allele_one.astype(jnp.int32) + allele_two.astype(jnp.int32)


def steps_of(rng, dims, cuts, least, top_value):
    def one(axis_at, blocks):
        draws = jax.random.uniform(jax.random.fold_in(jax.random.fold_in(rng, 6), axis_at), (blocks,), jnp.float32, least / len(cuts), top_value / len(cuts))
        return jnp.repeat(jnp.exp(draws), dims[axis_at] // blocks).reshape((-1,) + (1,) * (len(dims) - axis_at - 1))

    level = one(*cuts[0])
    for cut in cuts[1:]:
        level = level * one(*cut)
    return level


def split_up(number_of, total, bound, slope):
    portions = [(1 << 20) // math.isqrt(rank ** slope) + 1 for rank in range(2, number_of + 1)]
    surplus, holding = total - bound - (number_of - 1), [1] * (number_of - 1)
    while surplus > 0:
        movable = [i for i in range(number_of - 1) if holding[i] < bound]
        pool, budget = sum([portions[i] for i in movable]), surplus
        for i in movable:
            extra = min(bound - holding[i], max(1, budget * portions[i] // pool), surplus)
            holding[i] = holding[i] + extra
            surplus = surplus - extra
    return np.array([bound] + holding)


def uneven_parts(key, count, total, most, lean):
    if count == 2:
        one = jax.random.randint(key, (), max(1, total - most), min(most, total - 1) + 1)
        return jnp.stack([one, total - one])
    tallies = jnp.asarray(split_up(count, total, most, lean), jnp.int32)
    twos = (count - 1) // 2
    source_of, taker = tallies[1:1 + 2 * twos:2], tallies[2:2 + 2 * twos:2]
    room = jnp.minimum(source_of - 1, most - taker)
    moved = jax.random.randint(jax.random.fold_in(key, 1), (twos,), 0, 1 << 20) % (room + 1)
    tallies = tallies.at[1:1 + 2 * twos:2].set(source_of - moved).at[2:2 + 2 * twos:2].set(taker + moved)
    return tallies[jax.random.permutation(jax.random.fold_in(key, 2), count)]


def gaussian(rng, extent, spread, most, shards=(), kind=jnp.bfloat16):
    gain = steps_of(rng, extent, shards, -0.22, 0.18) if shards else 1.0
    entries = jax.random.normal(rng, extent, jnp.float32) * spread * gain
    return jnp.minimum(jnp.maximum(entries, -most), most).astype(kind)


def setup_inputs(seed: int = 0) -> dict:
    splits = jax.random.split(jax.random.key(seed), 5)
    return {
        "dosage": draw_dosage(jax.random.fold_in(splits[4], 71), 0),
        "phenotype": gaussian(splits[1], (SAMPLES,), 1.0, 6.0, ((0, 8),), jnp.float32),
        "perm_index": jax.vmap(lambda own: jax.random.permutation(own, SAMPLES))(jax.random.split(splits[2], PERMS)).reshape((PERMS, SAMPLES)).astype(jnp.int32),
        "seg_lengths": uneven_parts(splits[3], SEGS, V, SEG_MOST, 2).astype(jnp.int32),
    }


epsilon = 1e-05

def reference(dosage, phenotype, perm_index, seg_lengths):
    count_all = phenotype.shape[0]
    centered = phenotype - jnp.mean(phenotype)
    pheno_var = jnp.mean(centered * centered)
    rounded = centered.astype(jnp.bfloat16)
    allele_sum = lax.optimization_barrier(jnp.sum(dosage, axis=0)).astype(jnp.float32)
    allele_sq = lax.optimization_barrier(jnp.sum(dosage * dosage, axis=0)).astype(jnp.float32)
    allele_var = allele_sq / count_all - (allele_sum / count_all) ** 2
    dosage_bf = dosage.astype(jnp.bfloat16)
    block_rows = min(128, PERMS)
    grouped = perm_index.reshape(PERMS // block_rows, block_rows, count_all)

    def score_block(index_rows):
        permuted = jnp.take(rounded, index_rows, axis=0)
        return jnp.dot(permuted, dosage_bf, preferred_element_type=jnp.float32)
    score = lax.map(score_block, grouped).reshape(PERMS, dosage.shape[1])
    divisor = jnp.sqrt(count_all * (pheno_var + epsilon) * (allele_var + epsilon))
    zscore = score / divisor[None, :]
    prefix = lax.cummax(jnp.abs(zscore), axis=1)
    segment_end = (jnp.cumsum(seg_lengths) - 1).astype(jnp.int32)
    thresholds = jnp.take(prefix, segment_end, axis=1)
    return (zscore, thresholds)
```

```python
import jax
import jax.numpy as jnp
from jax import lax
from jax.experimental import pallas as pl
from jax.experimental.pallas import tpu as pltpu
from jax.sharding import PartitionSpec as P

epsilon = 1e-05
top = 32767.0


def in_order(blocks, dim):
    blocks = jnp.moveaxis(blocks, 0, dim)
    shape = blocks.shape
    return blocks.reshape(*shape[:dim], shape[dim] * shape[dim + 1], *shape[dim + 2 :])


def sent_to_all(value, axis):
    count = lax.axis_size(axis)
    return lax.all_to_all(
        jnp.broadcast_to(value[None], (count, *value.shape)), axis, 0, 0, tiled=True
    )


def collect(value, axis, dim):
    return in_order(sent_to_all(value, axis), dim)


def cut_along(value, dim, count):
    before, after = (value.shape[:dim], value.shape[dim + 1 :])
    return jnp.moveaxis(value.reshape(*before, count, -1, *after), dim, 0)


def sum_at_owner(value, axis, dim):
    count = lax.axis_size(axis)
    blocks = lax.all_to_all(cut_along(value, dim, count), axis, 0, 0, tiled=True)
    return jnp.sum(blocks, axis=0)


def looked_up(index, table_ref, half_at):
    high_half = index >= half_at
    word = jnp.where(high_half, index - half_at, index)
    lane = lax.bitwise_and(word, 127)
    row = lax.shift_right_logical(word, 7)
    rows = half_at // 128
    levels = max(1, (rows - 1).bit_length())
    bits = [lax.bitwise_and(row, 1 << k) != 0 for k in range(levels)]

    def pick(level, base):
        if level == 0:
            source = table_ref[pl.ds(base * 8, 8), :]
            return jnp.take_along_axis(source, lane, axis=1, mode="promise_in_bounds")
        low = pick(level - 1, base)
        if base + (1 << (level - 1)) >= rows:
            return low
        high = pick(level - 1, base + (1 << (level - 1)))
        return jnp.where(bits[level - 1], high, low)

    words = pick(levels, 0)
    low_part = lax.shift_right_arithmetic(lax.shift_left(words, 16), 16)
    return jnp.where(high_half, lax.shift_right_arithmetic(words, 16), low_part)


def gather_kernel(index_ref, table_ref, scale_ref, out_ref):
    rows, width = index_ref.shape
    half_at = table_ref.shape[0] // 8 * 128
    scale = scale_ref[0]

    @pl.loop(0, rows // 16)
    def _(r):
        @pl.loop(0, width // 128)
        def _(j):
            columns = pl.ds(pl.multiple_of(j * 128, 128), 128)
            parts = []
            for h in range(2):
                at = pl.ds(pl.multiple_of(r * 16 + 8 * h, 8), 8)
                picked = looked_up(index_ref[at, columns], table_ref, half_at)
                parts.append(picked.astype(jnp.float32) * scale)
            both = jnp.concatenate(parts, axis=0).astype(jnp.bfloat16)
            out_ref[pl.ds(pl.multiple_of(r * 16, 16), 16), columns] = both


def pick_traits(centered, perm_index):
    count_all = centered.shape[0]
    largest = jnp.max(jnp.abs(centered))
    unit = jnp.where(largest > 0, largest / top, 1.0)
    fixed = jnp.round(centered / unit).astype(jnp.int32)
    half = count_all // 2
    words = jnp.bitwise_or(jnp.bitwise_and(fixed[:half], 65535), fixed[half:] << 16)
    table = jnp.repeat(words.reshape(half // 128, 128), 8, axis=0)
    return pl.pallas_call(
        gather_kernel,
        out_shape=jax.ShapeDtypeStruct(perm_index.shape, jnp.bfloat16),
        in_specs=[
            pl.BlockSpec(memory_space=pltpu.VMEM),
            pl.BlockSpec(memory_space=pltpu.VMEM),
            pl.BlockSpec(memory_space=pltpu.SMEM),
        ],
        out_specs=pl.BlockSpec(memory_space=pltpu.VMEM),
    )(perm_index, table, unit.reshape(1))


def running_max(values):
    width = values.shape[1]
    offset = 1
    while offset < width:
        shifted = jnp.pad(values[:, : width - offset], ((0, 0), (offset, 0)))
        values = jnp.maximum(values, shifted)
        offset = offset * 2
    return values


def per_device(dosage, phenotype, perm_index, seg_lengths):
    pheno_all = collect(phenotype, "samp", 0)
    count_all = pheno_all.shape[0]
    centered = pheno_all - jnp.mean(pheno_all)
    pheno_var = jnp.mean(centered * centered)
    permuted = pick_traits(centered, perm_index)
    counts = jnp.stack([jnp.sum(dosage, axis=0), jnp.sum(dosage * dosage, axis=0)])
    counts = sent_to_all(counts.astype(jnp.float32), "samp").sum(axis=0)
    allele_var = counts[1] / count_all - (counts[0] / count_all) ** 2
    dosage_bf = dosage.astype(jnp.bfloat16)
    all_perms = lax.all_gather(permuted, "var", axis=0, tiled=True)
    score = sum_at_owner(
        jnp.dot(all_perms, dosage_bf, preferred_element_type=jnp.float32), "samp", 0
    )
    divisor = jnp.sqrt(count_all * (pheno_var + epsilon) * (allele_var + epsilon))
    zscore = score / divisor[None, :]
    local_prefix = running_max(jnp.abs(zscore))
    width = dosage.shape[1]
    segment_end = jnp.cumsum(seg_lengths) - 1
    local_end = jnp.minimum(segment_end - lax.axis_index("var") * width, width - 1)
    column_iota = lax.broadcasted_iota(jnp.int32, (width, local_end.shape[0]), 0)
    match = column_iota == local_end[None, :]
    picked = jnp.max(jnp.where(match[None, :, :], local_prefix[:, :, None], 0.0), axis=1)
    count = lax.axis_size("var")
    mine = lax.all_to_all(cut_along(picked, 0, count), "var", 0, 0, tiled=True).max(axis=0)
    thresholds = collect(mine, "var", 0)
    return (zscore, thresholds)


def solution(mesh):
    return jax.shard_map(
        per_device,
        mesh=mesh,
        in_specs=(P("samp", "var"), P("samp"), P("var", "samp"), P()),
        out_specs=(P("samp", "var"), P("samp", None)),
        check_vma=False,
    )
```

```python
import jax
import jax.numpy as jnp
from jax import lax
from jax.experimental import pallas as pl
from jax.experimental.pallas import tpu as pltpu
from jax.sharding import PartitionSpec as P

epsilon = 1e-05
top = 32767.0
side = 4
chunks = 4
rows = 16
parts = 4
pieces = 4
MESH = pl.DeviceIdType.MESH


def looked_up(index, table_ref, half_at):
    high_half = index >= half_at
    word = jnp.where(high_half, index - half_at, index)
    lane = lax.bitwise_and(word, 127)
    row = lax.shift_right_logical(word, 7)
    count = half_at // 128
    levels = max(1, (count - 1).bit_length())
    bits = [lax.bitwise_and(row, 1 << k) != 0 for k in range(levels)]

    def pick(level, base):
        if level == 0:
            source = table_ref[pl.ds(base * 8, 8), :]
            return jnp.take_along_axis(source, lane, axis=1, mode="promise_in_bounds")
        low = pick(level - 1, base)
        if base + (1 << (level - 1)) >= count:
            return low
        high = pick(level - 1, base + (1 << (level - 1)))
        return jnp.where(bits[level - 1], high, low)

    words = pick(levels, 0)
    low_part = lax.shift_right_arithmetic(lax.shift_left(words, 16), 16)
    return jnp.where(high_half, lax.shift_right_arithmetic(words, 16), low_part)


def aligned(value, by):
    return pl.multiple_of(value, by)


def kernel(
    dosage_ref, pheno_ref, index_ref, seg_ref, zscore_ref, thresholds_ref,
    traits, words, table, index, counts, dose, permuted, score, arrived, stats, marks,
    best, best_x, best_xy, best_y,
    local_sem, barrier_pad, trait_send, trait_recv, stat_send, stat_recv, dose_send, dose_recv,
    pass_send, pass_recv, perm_send, perm_recv, score_send, score_recv,
    x_send, x_recv, y_send, y_recv,
):
    samples, width = dosage_ref.shape
    var, samp = lax.axis_index("var"), lax.axis_index("samp")
    x, y = var // side, var % side
    z, core = samp // 2, samp % 2
    all_samples = 8 * samples
    part = 2 * samples // parts
    is_source = y // 2 == core
    own_slot = x * 2 + y % 2
    write_slot = jnp.where(is_source, own_slot, 8)

    def at(dx=0, dy=0):
        return lax.rem(x + dx + side, side) * side + lax.rem(y + dy + side, side)

    def remote(src, dst, send, recv, to_var=None, to_samp=None):
        return pltpu.make_async_remote_copy(
            src_ref=src, dst_ref=dst, send_sem=send, recv_sem=recv,
            device_id={
                "var": var if to_var is None else to_var,
                "samp": samp if to_samp is None else to_samp,
            },
            device_id_type=MESH,
        )

    piece = samples // pieces
    read_pheno = pltpu.make_async_copy(pheno_ref, traits.at[samp], local_sem.at[0])
    read_index = pltpu.make_async_copy(index_ref, index, local_sem.at[1])
    read_seg = pltpu.make_async_copy(seg_ref, marks, local_sem.at[2])
    read_dose = [
        pltpu.make_async_copy(
            dosage_ref.at[pl.ds(i * piece, piece)], counts.at[pl.ds(i * piece, piece)],
            local_sem.at[3 + i],
        )
        for i in range(pieces)
    ]
    read_pheno.start()
    for copy in read_dose[:2]:
        copy.start()
    read_index.start()
    read_seg.start()
    for copy in read_dose[2:]:
        copy.start()

    barrier = pltpu.get_barrier_semaphore()
    samp_peers = [lax.rem(samp + d, 8) for d in range(1, 8)]
    for peer in samp_peers:
        pl.semaphore_signal(barrier, inc=1, device_id={"var": var, "samp": peer}, device_id_type=MESH)
    for d in range(1, side):
        for to in (at(dx=d), at(dy=d)):
            pl.semaphore_signal(barrier, inc=1, device_id={"var": to, "samp": samp}, device_id_type=MESH)
    read_pheno.wait()
    pl.semaphore_wait(barrier, 13)

    trait_copies = [
        remote(traits.at[samp], traits.at[samp], trait_send.at[d], trait_recv.at[d], to_samp=samp_peers[d])
        for d in range(7)
    ]
    for copy in trait_copies:
        copy.start()

    def dose_copy(i):
        at_rows = pl.ds(aligned(core * samples + i * piece, 16), piece)
        return remote(dose.at[at_rows], dose.at[at_rows], dose_send.at[i], dose_recv.at[i], to_samp=samp ^ 1)

    def convert(i):
        read_dose[i].wait()
        step = 32

        def body(r, sums):
            one, two = sums
            for h in range(step // 16):
                start = i * piece + r * step + 16 * h
                value = counts[pl.ds(aligned(start, 16), 16), :].astype(jnp.float32)
                dose[pl.ds(aligned(core * samples + start, 16), 16), :] = value.astype(jnp.bfloat16)
                one = one + (value[:8] + value[8:])
                two = two + (value[:8] * value[:8] + value[8:] * value[8:])
            return one, two

        zero = jnp.zeros((8, width), jnp.float32)
        one, two = lax.fori_loop(0, piece // step, body, (zero, zero))
        if i == 0:
            stats[samp] = jnp.zeros((8, width), jnp.float32)
        stats[samp, 0:1, :] += jnp.sum(one, axis=0, keepdims=True)
        stats[samp, 1:2, :] += jnp.sum(two, axis=0, keepdims=True)
        dose_copy(i).start()

    stat_copies = [
        remote(stats.at[samp], stats.at[samp], stat_send.at[d], stat_recv.at[d], to_samp=samp_peers[d])
        for d in range(7)
    ]

    convert(0)
    convert(1)

    for copy in trait_copies:
        copy.wait_recv()
    high = all_samples // 2 // 128

    values = traits[...].reshape(2 * high, 128)
    mean = jnp.sum(jnp.sum(values, axis=0, keepdims=True), axis=1, keepdims=True) / all_samples
    centered = values - mean
    square = jnp.sum(centered * centered, axis=0, keepdims=True)
    pheno_var = jnp.sum(square, axis=1, keepdims=True) / all_samples
    largest = jnp.max(jnp.max(jnp.abs(centered), axis=0, keepdims=True), axis=1, keepdims=True)
    unit = jnp.where(largest > 0, largest / top, 1.0)
    fixed = jnp.round(centered / unit).astype(jnp.int32)
    words[...] = jnp.bitwise_or(
        jnp.bitwise_and(fixed[:high], 65535), lax.shift_left(fixed[high:], 16)
    )
    for r in range(high):
        table[pl.ds(8 * r, 8), :] = jnp.broadcast_to(words[pl.ds(r, 1), :], (8, 128))
    scale = jnp.broadcast_to(unit, (8, 128))
    read_index.wait()

    def gather(k, half):
        tiles = samples // 128 // 2

        @pl.loop(0, tiles)
        def _(j):
            start = (half * tiles + j) * 128
            both = []
            for h in range(2):
                block = index[pl.ds(k * rows + 8 * h, 8), pl.ds(aligned(start, 128), 128)]
                both.append(looked_up(block, table, high * 128).astype(jnp.float32) * scale)
            permuted[k, write_slot, :, pl.ds(aligned(core * samples + start, 128), 128)] = (
                jnp.concatenate(both, axis=0).astype(jnp.bfloat16)
            )

    def lanes(q):
        return pl.ds(aligned(q * part, 128), part)

    def passed(k, half, from_core):
        q = 2 * from_core + half
        return remote(
            permuted.at[k, 8, :, lanes(q)], permuted.at[k, own_slot, :, lanes(q)],
            pass_send.at[k, half], pass_recv.at[k, half], to_samp=samp ^ 1,
        )

    def pass_on(k, half):
        @pl.when(jnp.logical_not(is_source))
        def _():
            passed(k, half, core).start()

    def moved(axis, by):
        return at(dx=by) if axis == 0 else at(dy=by)

    def sends(k, q, event, slot, directions):
        return [
            remote(
                permuted.at[k, slot, :, lanes(q)], permuted.at[k, slot, :, lanes(q)],
                perm_send.at[k, q, event + i], perm_recv.at[k, q, slot], to_var=moved(axis, by),
            )
            for i, (axis, by) in enumerate(directions)
        ]

    def recv(k, q, slot):
        remote(
            permuted.at[k, slot, :, lanes(q)], permuted.at[k, slot, :, lanes(q)],
            perm_send.at[k, q, 0], perm_recv.at[k, q, slot],
        ).wait_recv()

    def slot_of(dx, dy):
        sx, sy = lax.rem(x - dx + side, side), lax.rem(y - dy + side, side)
        return sx * 2 + lax.rem(sy, 2), sy // 2 == core

    def routes(q):
        return q % 2, (1 if q < 2 else -1)

    def stage(k, q, level, act):
        axis, way = routes(q)
        other = 1 - axis
        if level == 0:
            todo = [(0, 0, 0, [(axis, way), (axis, -way), (other, way), (other, -way)])]
        elif level == 1:
            todo = []
            event = 4
            for d in (way % side, -way % side, 2):
                ways = [(other, way), (other, -way)]
                if d == way % side:
                    ways = [(axis, way), *ways]
                todo.append(((d, 0) if axis == 0 else (0, d), event, ways))
                event += len(ways)
            todo = [(*where, event, ways) for where, event, ways in todo]
        elif level == 2:
            todo = []
            for i, d in enumerate((0, way % side, -way % side, 2)):
                where = (d, way % side) if axis == 0 else (way % side, d)
                todo.append((*where, 11 + i, [(other, way)]))
        else:
            todo = []
            for far in (-way % side, 2):
                for d in range(side):
                    todo.append((*((d, far) if axis == 0 else (far, d)), 0, []))
        for dy in dict.fromkeys(t[1] for t in todo):

            @pl.when(slot_of(0, dy)[1])
            def _(dy=dy):
                for tx, ty, event, ways in todo:
                    if ty == dy:
                        act(k, q, level, slot_of(tx, ty)[0], event, ways)

    def go(k, q, level, slot, event, ways):
        if level:
            recv(k, q, slot)
        for copy in sends(k, q, event, slot, ways):
            copy.start()

    def done(k, q, level, slot, event, ways):
        for copy in sends(k, q, event, slot, ways):
            copy.wait_send()

    def stages(k, level, act=go):
        for q in range(parts):
            stage(k, q, level, act)

    def send_own(k, half):
        for q in range(parts):
            if q % 2 == half:

                @pl.when(jnp.logical_and(is_source, q // 2 == core))
                def _(q=q):
                    stage(k, q, 0, go)

    def send_passed(k, half):
        @pl.when(is_source)
        def _():
            passed(k, half, 1 - core).wait_recv()

        for q in range(parts):
            if q % 2 == half:

                @pl.when(jnp.logical_and(is_source, q // 2 != core))
                def _(q=q):
                    stage(k, q, 0, go)

    def multiply(k):
        @pl.loop(0, parts)
        def _(q):
            left = permuted[k, pl.ds(0, 8), :, lanes(q)].reshape(8 * rows, part)
            product = jnp.dot(
                left, dose[pl.ds(aligned(q * part, 16), part), :], preferred_element_type=jnp.float32
            )

            @pl.when(q == 0)
            def _():
                score[k] = product

            @pl.when(q > 0)
            def _():
                score[k] += product

    def score_copies(k):
        copies = []
        for d in (1, 3, 2):
            to = lax.rem(z + d, side)
            copies.append(
                remote(
                    score.at[k, pl.ds(aligned(to * 2 * rows, 2 * rows), 2 * rows)],
                    arrived.at[k, d - 1], score_send.at[k, d - 1], score_recv.at[k, d - 1],
                    to_samp=to * 2 + core,
                )
            )
        return copies

    def inverse_divisor():
        for copy in stat_copies:
            copy.wait_recv()
        sums = jnp.sum(stats[...], axis=0)
        allele_sum, allele_sq = sums[0:1], sums[1:2]
        allele_var = allele_sq / all_samples - (allele_sum / all_samples) ** 2
        return 1.0 / jnp.sqrt(all_samples * (pheno_var + epsilon) * (allele_var + epsilon))

    lane = lax.broadcasted_iota(jnp.int32, (2 * rows, 128), 1)

    def local_ends():
        ends = jnp.broadcast_to(marks[...], (8, 128))
        lane8 = lax.broadcasted_iota(jnp.int32, (8, 128), 1)
        offset = 1
        while offset < 128:
            ends = ends + jnp.where(lane8 >= offset, pltpu.roll(ends, offset, axis=1), 0)
            offset *= 2
        return ends - 1 - var * width

    def finish(k, inverse, ends):
        for copy in score_copies(k):
            copy.wait_recv()
        total = score[k, pl.ds(aligned(z * 2 * rows, 2 * rows), 2 * rows), :]
        for d in range(3):
            total = total + arrived[k, d]
        result = total * inverse
        zscore_ref[pl.ds(rows * k, rows), :] = result[:rows]
        zscore_ref[pl.ds(64 + rows * k, rows), :] = result[rows:]
        size = jnp.abs(result)
        best_here = jnp.zeros((2 * rows, 128), jnp.float32)
        for t in range(width // 128):
            run = size[:, 128 * t : 128 * (t + 1)]
            offset = 1
            while offset < 128:
                run = jnp.maximum(run, jnp.where(lane >= offset, pltpu.roll(run, offset, axis=1), 0.0))
                offset *= 2
            here = ends - 128 * t
            source = jnp.minimum(jnp.maximum(here, 0), 127)
            found = jnp.concatenate(
                [
                    jnp.where(
                        here >= 0,
                        jnp.take_along_axis(run[8 * g : 8 * g + 8], source, axis=1, mode="promise_in_bounds"),
                        0.0,
                    )
                    for g in range(2 * rows // 8)
                ],
                axis=0,
            )
            best_here = jnp.maximum(best_here, found)
        best[k] = best_here

    def best_copies(k, axis):
        source, target = (best, best_x) if axis == 0 else (best_xy, best_y)
        send, recv_sem = (x_send, x_recv) if axis == 0 else (y_send, y_recv)
        return [
            remote(source.at[k], target.at[k, d - 1], send.at[k, d - 1], recv_sem.at[k, d - 1], to_var=moved(axis, d))
            for d in (1, 3, 2)
        ]

    def join_x(k):
        for copy in best_copies(k, 0):
            copy.wait_recv()
        value = best[k]
        for d in range(3):
            value = jnp.maximum(value, best_x[k, d])
        best_xy[k] = value

    def join_y(k):
        for copy in best_copies(k, 1):
            copy.wait_recv()
        value = best_xy[k]
        for d in range(3):
            value = jnp.maximum(value, best_y[k, d])
        thresholds_ref[pl.ds(rows * k, rows), :] = value[:rows]
        thresholds_ref[pl.ds(64 + rows * k, rows), :] = value[rows:]

    def start(copies):
        for copy in copies:
            copy.start()

    for half in range(2):
        gather(0, half)
        pass_on(0, half)
        send_own(0, half)
    for half in range(2):
        send_passed(0, half)
    convert(2)
    convert(3)
    start(stat_copies)
    stages(0, 1)
    for k in range(1, chunks):
        gather(k, 0)
        pass_on(k, 0)
        send_own(k, 0)
        stages(k - 1, 2)
        gather(k, 1)
        pass_on(k, 1)
        send_own(k, 1)
        for half in range(2):
            send_passed(k, half)
        stages(k, 1)
        stages(k - 1, 3)
        if k == 1:
            for i in range(pieces):
                dose_other = pl.ds(aligned((1 - core) * samples + i * piece, 16), piece)
                remote(dose.at[dose_other], dose.at[dose_other], dose_send.at[i], dose_recv.at[i]).wait_recv()
            read_seg.wait()
        multiply(k - 1)
        start(score_copies(k - 1))
        if k == 2:
            inverse = inverse_divisor()
            ends = local_ends()
        if k >= 2:
            finish(k - 2, inverse, ends)
    last = chunks - 1
    stages(last, 2)
    stages(last, 3)
    multiply(last)
    start(score_copies(last))
    finish(last - 1, inverse, ends)
    for k in range(last):
        start(best_copies(k, 0))
    for k in range(last):
        join_x(k)
        start(best_copies(k, 1))
    finish(last, inverse, ends)
    start(best_copies(last, 0))
    for k in range(last):
        join_y(k)
    for copy in trait_copies + stat_copies + [dose_copy(i) for i in range(pieces)]:
        copy.wait_send()
    for k in range(chunks):
        for level in range(3):
            if level == 0:

                @pl.when(is_source)
                def _(k=k):
                    stages(k, 0, done)

                @pl.when(jnp.logical_not(is_source))
                def _(k=k):
                    for half in range(2):
                        passed(k, half, core).wait_send()

            else:
                stages(k, level, done)
        for copy in score_copies(k):
            copy.wait_send()
    join_x(last)
    start(best_copies(last, 1))
    join_y(last)
    for k in range(chunks):
        for copy in best_copies(k, 0) + best_copies(k, 1):
            copy.wait_send()


def per_device(dosage, phenotype, perm_index, seg_lengths):
    samples, width = dosage.shape
    segments = seg_lengths.shape[0]
    dma = pltpu.SemaphoreType.DMA
    f32, i32, bf16 = jnp.float32, jnp.int32, jnp.bfloat16
    vmem = pltpu.VMEM
    any_space = pl.BlockSpec(memory_space=pl.ANY)
    return pl.pallas_call(
        kernel,
        out_shape=(
            jax.ShapeDtypeStruct((128, width), f32),
            jax.ShapeDtypeStruct((128, segments), f32),
        ),
        in_specs=[any_space] * 4,
        out_specs=(pl.BlockSpec(memory_space=vmem), pl.BlockSpec(memory_space=vmem)),
        scratch_shapes=[
            vmem((8, samples // 128, 128), f32),
            vmem((samples * 4 // 128, 128), i32),
            vmem((samples * 4 // 16, 128), i32),
            vmem(perm_index.shape, i32),
            vmem((samples, width), i32),
            vmem((2 * samples, width), bf16),
            vmem((chunks, 9, rows, 2 * samples), bf16),
            vmem((chunks, 8 * rows, width), f32),
            vmem((chunks, 3, 2 * rows, width), f32),
            vmem((8, 8, width), f32),
            vmem((1, segments), i32),
            vmem((chunks, 2 * rows, segments), f32),
            vmem((chunks, 3, 2 * rows, segments), f32),
            vmem((chunks, 2 * rows, segments), f32),
            vmem((chunks, 3, 2 * rows, segments), f32),
            dma((3 + pieces,)),
            dma((1,)),
            dma((7,)),
            dma((7,)),
            dma((7,)),
            dma((7,)),
            dma((pieces,)),
            dma((pieces,)),
            dma((chunks, 2)),
            dma((chunks, 2)),
            dma((chunks, parts, 15)),
            dma((chunks, parts, 8)),
            dma((chunks, 3)),
            dma((chunks, 3)),
            dma((chunks, 3)),
            dma((chunks, 3)),
            dma((chunks, 3)),
            dma((chunks, 3)),
        ],
        compiler_params=pltpu.CompilerParams(
            collective_id=0, has_side_effects=True, vmem_limit_bytes=60 * 1024 * 1024
        ),
    )(
        dosage,
        phenotype.reshape(samples // 128, 128),
        perm_index,
        seg_lengths.reshape(1, segments),
    )


def solution(mesh):
    return jax.shard_map(
        per_device,
        mesh=mesh,
        in_specs=(P("samp", "var"), P("samp"), P("var", "samp"), P()),
        out_specs=(P("samp", "var"), P("samp", None)),
        check_vma=False,
    )
```

```python
import jax
import jax.numpy as jnp
from jax import lax
from jax.experimental import pallas as pl
from jax.experimental.pallas import tpu as pltpu
from jax.sharding import PartitionSpec as P

epsilon = 1e-05
top = 32767.0
side = 4
chunks = 4
rows = 16
parts = 4
pieces = 4
group = 2
MESH = pl.DeviceIdType.MESH

order = [
    ("gather", 0), ("gather", 1), ("gather", 2), ("own", 0, 0), ("gather", 3), ("gather", 4),
    ("passed", 0, 0), ("gather", 5), ("own", 0, 1), ("gather", 6), ("ring", 0, 0), ("passed", 0, 1),
    ("gather", 7), ("gather", 8), ("own", 1, 0), ("ring", 0, 2), ("gather", 9), ("ring", 0, 1),
    ("passed", 1, 0), ("gather", 10), ("far", 0, 0), ("gather", 11), ("own", 1, 1), ("passed", 1, 1),
    ("ring", 1, 0), ("side", 0, 0), ("ring", 0, 3), ("far", 0, 2), ("gather", 12), ("gather", 13),
    ("ring", 1, 2), ("gather", 14), ("own", 2, 0), ("far", 0, 1), ("passed", 2, 0), ("gather", 15),
    ("side", 0, 2), ("far", 1, 0), ("side", 0, 3), ("ring", 1, 3), ("gather", 16), ("ring", 1, 1),
    ("far", 1, 2), ("gather", 17), ("own", 2, 1), ("side", 0, 1), ("far", 0, 3), ("side", 1, 0),
    ("passed", 2, 1), ("gather", 18), ("ring", 2, 2), ("gather", 19), ("ring", 2, 0), ("gather", 20),
    ("own", 3, 0), ("side", 1, 3), ("passed", 3, 0), ("corner", 0, 1), ("gather", 21), ("side", 1, 2),
    ("far", 1, 1), ("corner", 0, 3), ("gather", 22), ("ring", 2, 1), ("side", 1, 1), ("corner", 0, 0),
    ("corner", 1, 0), ("far", 1, 3), ("ring", 2, 3), ("corner", 0, 2), ("gather", 23), ("own", 3, 1),
    ("corner", 1, 1), ("far", 2, 0), ("passed", 3, 1), ("ring", 3, 0), ("ring", 3, 2), ("far", 2, 1),
    ("corner", 1, 3), ("far", 2, 3), ("ring", 3, 1), ("corner", 1, 2), ("end", 0, 0), ("far", 2, 2),
    ("side", 2, 0), ("side", 2, 1), ("end", 0, 1), ("ring", 3, 3), ("corner", 2, 0), ("side", 2, 2),
    ("multiply", 0, 0), ("multiply", 0, 1), ("side", 2, 3), ("end", 1, 0), ("end", 1, 1), ("far", 3, 2),
    ("corner", 2, 2), ("far", 3, 1), ("corner", 2, 1), ("far", 3, 0), ("far", 3, 3), ("corner", 2, 3),
    ("side", 3, 2), ("side", 3, 0), ("multiply", 1, 0), ("multiply", 1, 1), ("finish", 0), ("side", 3, 1),
    ("side", 3, 3), ("corner", 3, 2), ("corner", 3, 0), ("end", 2, 0), ("multiply", 2, 0), ("corner", 3, 3),
    ("corner", 3, 1), ("end", 2, 1), ("multiply", 2, 1), ("finish", 1), ("end", 3, 0), ("multiply", 3, 0),
    ("end", 3, 1), ("multiply", 3, 1), ("finish", 2),
]
straight_ring = ()
straight_side = ()


def looked_up(index, table_ref, half_at):
    high_half = index >= half_at
    word = jnp.where(high_half, index - half_at, index)
    lane = lax.bitwise_and(word, 127)
    row = lax.shift_right_logical(word, 7)
    count = half_at // 128
    levels = max(1, (count - 1).bit_length())
    bits = [lax.bitwise_and(row, 1 << k) != 0 for k in range(levels)]

    def pick(level, base):
        if level == 0:
            source = table_ref[pl.ds(base * 8, 8), :]
            return jnp.take_along_axis(source, lane, axis=1, mode="promise_in_bounds")
        low = pick(level - 1, base)
        if base + (1 << (level - 1)) >= count:
            return low
        high = pick(level - 1, base + (1 << (level - 1)))
        return jnp.where(bits[level - 1], high, low)

    words = pick(levels, 0)
    low_part = lax.shift_right_arithmetic(lax.shift_left(words, 16), 16)
    return jnp.where(high_half, lax.shift_right_arithmetic(words, 16), low_part)


def aligned(value, by):
    return pl.multiple_of(value, by)


def kernel(
    dosage_ref, pheno_ref, index_ref, seg_ref, zscore_ref, thresholds_ref,
    traits, words, table, index, counts, dose, permuted, score, arrived, stats, marks,
    best, best_x, best_xy, best_y,
    local_sem, trait_send, trait_recv, stat_send, stat_recv, dose_send, dose_recv,
    pass_send, pass_recv, perm_send, perm_recv, score_send, score_recv,
    x_send, x_recv, y_send, y_recv,
):
    samples, width = dosage_ref.shape
    var, samp = lax.axis_index("var"), lax.axis_index("samp")
    x, y = var // side, var % side
    z, core = samp // 2, samp % 2
    all_samples = 8 * samples
    part = 2 * samples // parts
    is_source = y // 2 == core
    own_slot = x * 2 + y % 2
    write_slot = jnp.where(is_source, own_slot, 8)

    def at(dx=0, dy=0):
        return lax.rem(x + dx + side, side) * side + lax.rem(y + dy + side, side)

    def remote(src, dst, send, recv, to_var=None, to_samp=None):
        return pltpu.make_async_remote_copy(
            src_ref=src, dst_ref=dst, send_sem=send, recv_sem=recv,
            device_id={
                "var": var if to_var is None else to_var,
                "samp": samp if to_samp is None else to_samp,
            },
            device_id_type=MESH,
        )

    piece = samples // pieces
    read_pheno = pltpu.make_async_copy(pheno_ref, traits.at[samp], local_sem.at[0])
    read_index = pltpu.make_async_copy(index_ref, index, local_sem.at[1])
    read_seg = pltpu.make_async_copy(seg_ref, marks, local_sem.at[2])
    read_dose = [
        pltpu.make_async_copy(
            dosage_ref.at[pl.ds(i * piece, piece)], counts.at[pl.ds(i * piece, piece)],
            local_sem.at[3 + i],
        )
        for i in range(pieces)
    ]
    read_pheno.start()
    for copy in read_dose[:2]:
        copy.start()
    read_index.start()
    read_seg.start()
    for copy in read_dose[2:]:
        copy.start()

    barrier = pltpu.get_barrier_semaphore()
    samp_peers = [lax.rem(samp + d, 8) for d in range(1, 8)]
    for peer in samp_peers:
        pl.semaphore_signal(barrier, inc=1, device_id={"var": var, "samp": peer}, device_id_type=MESH)
    for d in range(1, side):
        for to in (at(dx=d), at(dy=d)):
            pl.semaphore_signal(barrier, inc=1, device_id={"var": to, "samp": samp}, device_id_type=MESH)
    trait_copies = [
        remote(traits.at[samp], traits.at[samp], trait_send.at[d], trait_recv.at[d], to_samp=samp_peers[d])
        for d in range(7)
    ]

    def dose_copy(i):
        at_rows = pl.ds(aligned(core * samples + i * piece, 16), piece)
        return remote(dose.at[at_rows], dose.at[at_rows], dose_send.at[i], dose_recv.at[i], to_samp=samp ^ 1)

    def convert(i):
        read_dose[i].wait()
        step = 32

        def body(r, sums):
            one, two = sums
            for h in range(step // 16):
                start = i * piece + r * step + 16 * h
                value = counts[pl.ds(aligned(start, 16), 16), :].astype(jnp.float32)
                dose[pl.ds(aligned(core * samples + start, 16), 16), :] = value.astype(jnp.bfloat16)
                one = one + (value[:8] + value[8:])
                two = two + (value[:8] * value[:8] + value[8:] * value[8:])
            return one, two

        zero = jnp.zeros((8, width), jnp.float32)
        one, two = lax.fori_loop(0, piece // step, body, (zero, zero))
        if i == 0:
            stats[samp] = jnp.zeros((8, width), jnp.float32)
        stats[samp, 0:1, :] += jnp.sum(one, axis=0, keepdims=True)
        stats[samp, 1:2, :] += jnp.sum(two, axis=0, keepdims=True)

    stat_copies = [
        remote(stats.at[samp], stats.at[samp], stat_send.at[d], stat_recv.at[d], to_samp=samp_peers[d])
        for d in range(7)
    ]

    for i in range(pieces):
        convert(i)
    read_pheno.wait()
    pl.semaphore_wait(barrier, 13)
    for copy in trait_copies:
        copy.start()

    for copy in trait_copies:
        copy.wait_recv()
    high = all_samples // 2 // 128

    values = traits[...].reshape(2 * high, 128)
    mean = jnp.sum(jnp.sum(values, axis=0, keepdims=True), axis=1, keepdims=True) / all_samples
    centered = values - mean
    square = jnp.sum(centered * centered, axis=0, keepdims=True)
    pheno_var = jnp.sum(square, axis=1, keepdims=True) / all_samples
    largest = jnp.max(jnp.max(jnp.abs(centered), axis=0, keepdims=True), axis=1, keepdims=True)
    unit = jnp.where(largest > 0, largest / top, 1.0)
    fixed = jnp.round(centered / unit).astype(jnp.int32)
    words[...] = jnp.bitwise_or(
        jnp.bitwise_and(fixed[:high], 65535), lax.shift_left(fixed[high:], 16)
    )
    for r in range(high):
        table[pl.ds(8 * r, 8), :] = jnp.broadcast_to(words[pl.ds(r, 1), :], (8, 128))
    scale = jnp.broadcast_to(unit, (8, 128))
    read_index.wait()

    def gather(i):
        k, first = i // 6, i % 6 * (samples // 128 // 6)

        @pl.loop(0, samples // 128 // 6 // group)
        def _(j):
            for t in range(group):
                start = (first + j * group + t) * 128
                both = []
                for h in range(2):
                    block = index[pl.ds(k * rows + 8 * h, 8), pl.ds(aligned(start, 128), 128)]
                    both.append(looked_up(block, table, high * 128).astype(jnp.float32) * scale)
                permuted[k, write_slot, :, pl.ds(aligned(core * samples + start, 128), 128)] = (
                    jnp.concatenate(both, axis=0).astype(jnp.bfloat16)
                )

    def lanes(q):
        return pl.ds(aligned(q * part, 128), part)

    def passed(k, half, from_core):
        q = 2 * from_core + half
        return remote(
            permuted.at[k, 8, :, lanes(q)], permuted.at[k, own_slot, :, lanes(q)],
            pass_send.at[k, half], pass_recv.at[k, half], to_samp=samp ^ 1,
        )

    def pass_on(k, half):
        @pl.when(jnp.logical_not(is_source))
        def _():
            passed(k, half, core).start()

    def moved(axis, by):
        return at(dx=by) if axis == 0 else at(dy=by)

    def sends(k, q, event, slot, directions):
        return [
            remote(
                permuted.at[k, slot, :, lanes(q)], permuted.at[k, slot, :, lanes(q)],
                perm_send.at[k, q, event + i], perm_recv.at[k, q, slot], to_var=moved(axis, by),
            )
            for i, (axis, by) in enumerate(directions)
        ]

    def recv(k, q, slot):
        remote(
            permuted.at[k, slot, :, lanes(q)], permuted.at[k, slot, :, lanes(q)],
            perm_send.at[k, q, 0], perm_recv.at[k, q, slot],
        ).wait_recv()

    def slot_of(dx, dy):
        sx, sy = lax.rem(x - dx + side, side), lax.rem(y - dy + side, side)
        return sx * 2 + lax.rem(sy, 2), sy // 2 == core

    def routes(q):
        return q % 2, (1 if q < 2 else -1)

    def cells(k, q, level):
        axis, way = routes(q)
        other = 1 - axis
        unit_no = 2 * k + q % 2
        straight = unit_no in straight_ring
        both = [(other, way), (other, -way)]
        if unit_no in straight_side:
            both.append((other, 2 * way))
        near, back = way % side, -way % side
        if level == "own":
            ring = [(axis, way), (axis, -way)] + [(axis, 2 * way)] * straight
            found = [(0, 0, 0, ring + both)]
        elif level == "ring":
            found = [(near, 0, 6, [(axis, way)] * (not straight) + both), (back, 0, 10, both)]
        elif level == "far":
            found = [(2, 0, 13, both)]
        elif unit_no in straight_side:
            ends = level == "end"
            found = [(d, s, 0, []) for s in (near, back, 2) for d in range(side) if ends]
        elif level == "side":
            found = [(d, near, 16 + i, [(other, way)]) for i, d in enumerate((0, near, back))]
        elif level == "corner":
            found = [(2, near, 19, [(other, way)])]
        else:
            found = [(d, s, 0, []) for s in (back, 2) for d in range(side)]
        return [(p, s, *rest) if axis == 0 else (s, p, *rest) for p, s, *rest in found]

    def stage(k, q, level, act):
        todo = cells(k, q, level)
        for dy in dict.fromkeys(t[1] for t in todo):

            @pl.when(slot_of(0, dy)[1])
            def _(dy=dy):
                for tx, ty, event, ways in todo:
                    if ty == dy:
                        act(k, q, level, slot_of(tx, ty)[0], event, ways)

    def go(k, q, level, slot, event, ways):
        if level != "own":
            recv(k, q, slot)
        for copy in sends(k, q, event, slot, ways):
            copy.start()

    def done(k, q, level, slot, event, ways):
        for copy in sends(k, q, event, slot, ways):
            copy.wait_send()

    def send_own(k, half):
        for q in range(parts):
            if q % 2 == half:

                @pl.when(jnp.logical_and(is_source, q // 2 == core))
                def _(q=q):
                    stage(k, q, "own", go)

    def send_passed(k, half):
        @pl.when(is_source)
        def _():
            passed(k, half, 1 - core).wait_recv()

        for q in range(parts):
            if q % 2 == half:

                @pl.when(jnp.logical_and(is_source, q // 2 != core))
                def _(q=q):
                    stage(k, q, "own", go)

    def multiply(k, half):
        @pl.loop(0, parts // 2)
        def _(i):
            q = 2 * i + half
            left = permuted[k, pl.ds(0, 8), :, lanes(q)].reshape(8 * rows, part)
            product = jnp.dot(
                left, dose[pl.ds(aligned(q * part, 16), part), :], preferred_element_type=jnp.float32
            )
            if half:
                score[k] += product
            else:

                @pl.when(i == 0)
                def _():
                    score[k] = product

                @pl.when(i > 0)
                def _():
                    score[k] += product

    def score_copies(k):
        copies = []
        for d in (1, 3, 2):
            to = lax.rem(z + d, side)
            copies.append(
                remote(
                    score.at[k, pl.ds(aligned(to * 2 * rows, 2 * rows), 2 * rows)],
                    arrived.at[k, d - 1], score_send.at[k, d - 1], score_recv.at[k, d - 1],
                    to_samp=to * 2 + core,
                )
            )
        return copies

    def inverse_divisor():
        for copy in stat_copies:
            copy.wait_recv()
        sums = jnp.sum(stats[...], axis=0)
        allele_sum, allele_sq = sums[0:1], sums[1:2]
        allele_var = allele_sq / all_samples - (allele_sum / all_samples) ** 2
        return 1.0 / jnp.sqrt(all_samples * (pheno_var + epsilon) * (allele_var + epsilon))

    lane = lax.broadcasted_iota(jnp.int32, (2 * rows, 128), 1)

    def local_ends():
        ends = jnp.broadcast_to(marks[...], (8, 128))
        lane8 = lax.broadcasted_iota(jnp.int32, (8, 128), 1)
        offset = 1
        while offset < 128:
            ends = ends + jnp.where(lane8 >= offset, pltpu.roll(ends, offset, axis=1), 0)
            offset *= 2
        return ends - 1 - var * width

    def finish(k, inverse, ends):
        for copy in score_copies(k):
            copy.wait_recv()
        total = score[k, pl.ds(aligned(z * 2 * rows, 2 * rows), 2 * rows), :]
        for d in range(3):
            total = total + arrived[k, d]
        result = total * inverse
        zscore_ref[pl.ds(rows * k, rows), :] = result[:rows]
        zscore_ref[pl.ds(64 + rows * k, rows), :] = result[rows:]
        size = jnp.abs(result)
        best_here = jnp.zeros((2 * rows, 128), jnp.float32)
        for t in range(width // 128):
            run = size[:, 128 * t : 128 * (t + 1)]
            offset = 1
            while offset < 128:
                run = jnp.maximum(run, jnp.where(lane >= offset, pltpu.roll(run, offset, axis=1), 0.0))
                offset *= 2
            here = ends - 128 * t
            source = jnp.minimum(jnp.maximum(here, 0), 127)
            found = jnp.concatenate(
                [
                    jnp.where(
                        here >= 0,
                        jnp.take_along_axis(run[8 * g : 8 * g + 8], source, axis=1, mode="promise_in_bounds"),
                        0.0,
                    )
                    for g in range(2 * rows // 8)
                ],
                axis=0,
            )
            best_here = jnp.maximum(best_here, found)
        best[k] = best_here

    def best_copies(k, axis):
        source, target = (best, best_x) if axis == 0 else (best_xy, best_y)
        send, recv_sem = (x_send, x_recv) if axis == 0 else (y_send, y_recv)
        return [
            remote(source.at[k], target.at[k, d - 1], send.at[k, d - 1], recv_sem.at[k, d - 1], to_var=moved(axis, d))
            for d in (1, 3, 2)
        ]

    def join_x(k):
        for copy in best_copies(k, 0):
            copy.wait_recv()
        value = best[k]
        for d in range(3):
            value = jnp.maximum(value, best_x[k, d])
        best_xy[k] = value

    def join_y(k):
        for copy in best_copies(k, 1):
            copy.wait_recv()
        value = best_xy[k]
        for d in range(3):
            value = jnp.maximum(value, best_y[k, d])
        thresholds_ref[pl.ds(rows * k, rows), :] = value[:rows]
        thresholds_ref[pl.ds(64 + rows * k, rows), :] = value[rows:]

    def start(copies):
        for copy in copies:
            copy.start()

    def wait_dose():
        for i in range(pieces):
            theirs = pl.ds(aligned((1 - core) * samples + i * piece, 16), piece)
            remote(dose.at[theirs], dose.at[theirs], dose_send.at[i], dose_recv.at[i]).wait_recv()

    def drain_passed(k):
        @pl.when(jnp.logical_not(is_source))
        def _():
            for half in range(2):
                passed(k, half, core).wait_send()

    last = chunks - 1
    sent, finished, started = False, [], []
    last_send = [e for e in order if e[0] in ("ring", "far", "side", "corner")][-1]
    for name, *where in order:
        if name == "gather":
            gather(*where)
            if where[0] == 0:
                start([dose_copy(i) for i in range(pieces)] + stat_copies)
            if where[0] == 3:
                read_seg.wait()
                ends = local_ends()
        elif name == "own":
            pass_on(*where)
            send_own(*where)
        elif name == "passed":
            send_passed(*where)
        elif name == "end":
            k, half = where
            for q in range(half, parts, 2):
                stage(k, q, "end", go)
        elif name == "multiply":
            k, half = where
            if k == 0 and half == 0:
                wait_dose()
                inverse = inverse_divisor()
            multiply(k, half)
            if half:
                start(score_copies(k))
        elif name == "finish":
            finish(*where, inverse, ends)
            finished.extend(where)
        else:
            stage(*where, name, go)
        if (name, *where) == last_send:
            sent = True
        while sent and len(started) < len(finished):
            started.append(finished[len(started)])
            start(best_copies(started[-1], 0))
    for k in range(last - 1):
        join_x(k)
        start(best_copies(k, 1))
    finish(last, inverse, ends)
    start(best_copies(last, 0))
    join_x(last - 1)
    start(best_copies(last - 1, 1))
    for copy in trait_copies + stat_copies + [dose_copy(i) for i in range(pieces)]:
        copy.wait_send()
    for k in range(chunks):
        drain_passed(k)
        for q in range(parts):
            for level in ("own", "ring", "far", "side", "corner"):
                stage(k, q, level, done)
        for copy in score_copies(k):
            copy.wait_send()
    join_x(last)
    start(best_copies(last, 1))
    for k in range(chunks):
        join_y(k)
    for k in range(chunks):
        for copy in best_copies(k, 0) + best_copies(k, 1):
            copy.wait_send()


def keep_kernel(zscore_ref, thresholds_ref, zscore_out, thresholds_out, first, second, sem):
    into = [
        pltpu.make_async_copy(zscore_ref, first, sem.at[0]),
        pltpu.make_async_copy(thresholds_ref, second, sem.at[1]),
    ]
    out = [
        pltpu.make_async_copy(first, zscore_out, sem.at[2]),
        pltpu.make_async_copy(second, thresholds_out, sem.at[3]),
    ]
    for copy in into:
        copy.start()
    for copy, after in zip(into, out):
        copy.wait()
        after.start()
    for copy in out:
        copy.wait()


def per_device(dosage, phenotype, perm_index, seg_lengths):
    samples, width = dosage.shape
    segments = seg_lengths.shape[0]
    dma = pltpu.SemaphoreType.DMA
    f32, i32, bf16 = jnp.float32, jnp.int32, jnp.bfloat16
    vmem = pltpu.VMEM
    any_space = pl.BlockSpec(memory_space=pltpu.HBM)
    outs = (
        jax.ShapeDtypeStruct((128, width), f32),
        jax.ShapeDtypeStruct((128, segments), f32),
    )
    zscore, thresholds = pl.pallas_call(
        kernel,
        out_shape=outs,
        in_specs=[any_space] * 4,
        out_specs=(pl.BlockSpec(memory_space=vmem), pl.BlockSpec(memory_space=vmem)),
        scratch_shapes=[
            vmem((8, samples // 128, 128), f32),
            vmem((samples * 4 // 128, 128), i32),
            vmem((samples * 4 // 16, 128), i32),
            vmem(perm_index.shape, i32),
            vmem((samples, width), i32),
            vmem((2 * samples, width), bf16),
            vmem((chunks, 9, rows, 2 * samples), bf16),
            vmem((chunks, 8 * rows, width), f32),
            vmem((chunks, 3, 2 * rows, width), f32),
            vmem((8, 8, width), f32),
            vmem((1, segments), i32),
            vmem((chunks, 2 * rows, segments), f32),
            vmem((chunks, 3, 2 * rows, segments), f32),
            vmem((chunks, 2 * rows, segments), f32),
            vmem((chunks, 3, 2 * rows, segments), f32),
            dma((3 + pieces,)),
            dma((7,)),
            dma((7,)),
            dma((7,)),
            dma((7,)),
            dma((pieces,)),
            dma((pieces,)),
            dma((chunks, 2)),
            dma((chunks, 2)),
            dma((chunks, parts, 20)),
            dma((chunks, parts, 8)),
            dma((chunks, 3)),
            dma((chunks, 3)),
            dma((chunks, 3)),
            dma((chunks, 3)),
            dma((chunks, 3)),
            dma((chunks, 3)),
        ],
        compiler_params=pltpu.CompilerParams(
            collective_id=0, has_side_effects=True, vmem_limit_bytes=60 * 1024 * 1024
        ),
    )(
        dosage,
        phenotype.reshape(samples // 128, 128),
        perm_index,
        seg_lengths.reshape(1, segments),
    )
    return pl.pallas_call(
        keep_kernel,
        out_shape=outs,
        in_specs=[any_space] * 2,
        out_specs=(any_space, any_space),
        scratch_shapes=[vmem((128, width), f32), vmem((128, segments), f32), dma((4,))],
        compiler_params=pltpu.CompilerParams(vmem_limit_bytes=60 * 1024 * 1024),
    )(zscore, thresholds)


def solution(mesh):
    return jax.shard_map(
        per_device,
        mesh=mesh,
        in_specs=(P("samp", "var"), P("samp"), P("var", "samp"), P()),
        out_specs=(P("samp", "var"), P("samp", None)),
        check_vma=False,
    )
```

```python
import jax
import jax.numpy as jnp
from jax import lax
from jax.experimental import pallas as pl
from jax.experimental.pallas import tpu as pltpu
from jax.sharding import PartitionSpec as P

epsilon = 1e-05
top = 32767.0
side = 4
chunks = 4
rows = 16
parts = 4
pieces = 4
group = 2
MESH = pl.DeviceIdType.MESH

order = [
    ("gather", 0), ("gather", 1), ("gather", 2), ("own", 0, 0), ("gather", 3), ("gather", 4), ("gather", 5),
    ("own", 0, 1), ("gather", 6), ("gather", 7), ("passed", 0, 0), ("passed", 0, 1), ("gather", 8),
    ("ring", 0, 0), ("own", 1, 0), ("gather", 9), ("passed", 1, 0), ("gather", 10), ("gather", 11),
    ("own", 1, 1), ("ring", 0, 1), ("gather", 12), ("passed", 1, 1), ("ring", 0, 2), ("gather", 13),
    ("ring", 0, 3), ("ring", 1, 0), ("gather", 14), ("own", 2, 0), ("side", 0, 0), ("ring", 1, 2),
    ("passed", 2, 0), ("gather", 15), ("far", 0, 0), ("gather", 16), ("gather", 17), ("own", 2, 1),
    ("passed", 2, 1), ("ring", 1, 1), ("far", 0, 1), ("side", 0, 1), ("far", 0, 2), ("gather", 18),
    ("side", 0, 2), ("side", 0, 3), ("far", 1, 0), ("gather", 19), ("ring", 1, 3), ("ring", 2, 2),
    ("gather", 20), ("own", 3, 0), ("gather", 21), ("ring", 2, 0), ("passed", 3, 0), ("gather", 22),
    ("far", 0, 3), ("corner", 0, 1), ("corner", 0, 0), ("gather", 23), ("ring", 2, 3), ("own", 3, 1),
    ("ring", 2, 1), ("far", 1, 1), ("passed", 3, 1), ("far", 1, 2), ("far", 1, 3), ("corner", 0, 2),
    ("side", 1, 2), ("side", 1, 0), ("corner", 0, 3), ("ring", 3, 0), ("far", 2, 3), ("ring", 3, 2),
    ("ring", 3, 1), ("far", 2, 1), ("ring", 3, 3), ("far", 2, 0), ("side", 1, 1), ("end", 0, 0),
    ("side", 1, 3), ("far", 2, 2), ("multiply", 0, 0), ("corner", 1, 0), ("corner", 1, 2), ("far", 3, 0),
    ("end", 0, 1), ("far", 3, 2), ("side", 2, 0), ("corner", 1, 1), ("multiply", 0, 1), ("corner", 1, 3),
    ("side", 2, 2), ("far", 3, 1), ("corner", 2, 0), ("side", 2, 1), ("side", 3, 0), ("far", 3, 3),
    ("side", 2, 3), ("corner", 2, 1), ("corner", 2, 3), ("corner", 2, 2), ("side", 3, 2), ("end", 1, 0),
    ("multiply", 1, 0), ("side", 3, 3), ("corner", 3, 2), ("end", 1, 1), ("corner", 3, 0), ("side", 3, 1),
    ("multiply", 1, 1), ("corner", 3, 1), ("corner", 3, 3), ("end", 2, 0), ("multiply", 2, 0), ("end", 2, 1),
    ("multiply", 2, 1), ("finish", 0), ("end", 3, 0), ("multiply", 3, 0), ("end", 3, 1), ("multiply", 3, 1),
    ("finish", 1), ("finish", 2),
]
straight_ring = ()
straight_side = ()


def looked_up(index, table_ref, half_at):
    high_half = index >= half_at
    word = jnp.where(high_half, index - half_at, index)
    lane = lax.bitwise_and(word, 127)
    row = lax.shift_right_logical(word, 7)
    count = half_at // 128
    levels = max(1, (count - 1).bit_length())
    bits = [lax.bitwise_and(row, 1 << k) != 0 for k in range(levels)]

    def pick(level, base):
        if level == 0:
            source = table_ref[pl.ds(base * 8, 8), :]
            return jnp.take_along_axis(source, lane, axis=1, mode="promise_in_bounds")
        low = pick(level - 1, base)
        if base + (1 << (level - 1)) >= count:
            return low
        high = pick(level - 1, base + (1 << (level - 1)))
        return jnp.where(bits[level - 1], high, low)

    words = pick(levels, 0)
    low_part = lax.shift_right_arithmetic(lax.shift_left(words, 16), 16)
    return jnp.where(high_half, lax.shift_right_arithmetic(words, 16), low_part)


def aligned(value, by):
    return pl.multiple_of(value, by)


def kernel(
    dosage_ref, pheno_ref, index_ref, seg_ref, zscore_ref, thresholds_ref,
    traits, words, table, index, counts, dose, permuted, score, row_sum, leaving, arrived, stats, marks,
    best, best_x, best_xy, best_y,
    local_sem, trait_send, trait_recv, stat_send, stat_recv, dose_send, dose_recv,
    pass_send, pass_recv, perm_send, perm_recv, score_send, score_recv,
    x_send, x_recv, y_send, y_recv,
):
    samples, width = dosage_ref.shape
    var, samp = lax.axis_index("var"), lax.axis_index("samp")
    x, y = var // side, var % side
    z, core = samp // 2, samp % 2
    all_samples = 8 * samples
    part = 2 * samples // parts
    is_source = y // 2 == core
    own_slot = x * 2 + y % 2
    write_slot = jnp.where(is_source, own_slot, 8)

    def at(dx=0, dy=0):
        return lax.rem(x + dx + side, side) * side + lax.rem(y + dy + side, side)

    def remote(src, dst, send, recv, to_var=None, to_samp=None):
        return pltpu.make_async_remote_copy(
            src_ref=src, dst_ref=dst, send_sem=send, recv_sem=recv,
            device_id={
                "var": var if to_var is None else to_var,
                "samp": samp if to_samp is None else to_samp,
            },
            device_id_type=MESH,
        )

    piece = samples // pieces
    read_pheno = pltpu.make_async_copy(pheno_ref, traits.at[samp], local_sem.at[0])
    read_index = pltpu.make_async_copy(index_ref, index, local_sem.at[1])
    read_seg = pltpu.make_async_copy(seg_ref, marks, local_sem.at[2])
    read_dose = [
        pltpu.make_async_copy(
            dosage_ref.at[pl.ds(i * piece, piece)], counts.at[pl.ds(i * piece, piece)],
            local_sem.at[3 + i],
        )
        for i in range(pieces)
    ]
    read_pheno.start()
    for copy in read_dose[:2]:
        copy.start()
    read_index.start()
    read_seg.start()
    for copy in read_dose[2:]:
        copy.start()

    barrier = pltpu.get_barrier_semaphore()
    samp_peers = [lax.rem(samp + d, 8) for d in range(1, 8)]
    for peer in samp_peers:
        pl.semaphore_signal(barrier, inc=1, device_id={"var": var, "samp": peer}, device_id_type=MESH)
    for d in range(1, side):
        for to in (at(dx=d), at(dy=d)):
            pl.semaphore_signal(barrier, inc=1, device_id={"var": to, "samp": samp}, device_id_type=MESH)
    trait_copies = [
        remote(traits.at[samp], traits.at[samp], trait_send.at[d], trait_recv.at[d], to_samp=samp_peers[d])
        for d in range(7)
    ]

    def dose_copy(i):
        at_rows = pl.ds(aligned(core * samples + i * piece, 16), piece)
        return remote(dose.at[at_rows], dose.at[at_rows], dose_send.at[i], dose_recv.at[i], to_samp=samp ^ 1)

    def convert(i):
        read_dose[i].wait()
        step = 32

        def body(r, sums):
            one, two = sums
            for h in range(step // 16):
                start = i * piece + r * step + 16 * h
                value = counts[pl.ds(aligned(start, 16), 16), :].astype(jnp.float32)
                dose[pl.ds(aligned(core * samples + start, 16), 16), :] = value.astype(jnp.bfloat16)
                one = one + (value[:8] + value[8:])
                two = two + (value[:8] * value[:8] + value[8:] * value[8:])
            return one, two

        zero = jnp.zeros((8, width), jnp.float32)
        one, two = lax.fori_loop(0, piece // step, body, (zero, zero))
        if i == 0:
            stats[samp] = jnp.zeros((8, width), jnp.float32)
        stats[samp, 0:1, :] += jnp.sum(one, axis=0, keepdims=True)
        stats[samp, 1:2, :] += jnp.sum(two, axis=0, keepdims=True)

    stat_copies = [
        remote(stats.at[samp], stats.at[samp], stat_send.at[d], stat_recv.at[d], to_samp=samp_peers[d])
        for d in range(7)
    ]

    for i in range(pieces):
        convert(i)
    read_pheno.wait()
    pl.semaphore_wait(barrier, 13)
    for copy in trait_copies:
        copy.start()

    for copy in trait_copies:
        copy.wait_recv()
    high = all_samples // 2 // 128

    values = traits[...].reshape(2 * high, 128)
    mean = jnp.sum(jnp.sum(values, axis=0, keepdims=True), axis=1, keepdims=True) / all_samples
    centered = values - mean
    square = jnp.sum(centered * centered, axis=0, keepdims=True)
    pheno_var = jnp.sum(square, axis=1, keepdims=True) / all_samples
    largest = jnp.max(jnp.max(jnp.abs(centered), axis=0, keepdims=True), axis=1, keepdims=True)
    unit = jnp.where(largest > 0, largest / top, 1.0)
    fixed = jnp.round(centered / unit).astype(jnp.int32)
    words[...] = jnp.bitwise_or(
        jnp.bitwise_and(fixed[:high], 65535), lax.shift_left(fixed[high:], 16)
    )
    for r in range(high):
        table[pl.ds(8 * r, 8), :] = jnp.broadcast_to(words[pl.ds(r, 1), :], (8, 128))
    held = (fixed.astype(jnp.float32) * unit).astype(jnp.bfloat16).astype(jnp.float32)
    held_sum = jnp.sum(jnp.sum(held, axis=0, keepdims=True), axis=1, keepdims=True)
    scale = jnp.broadcast_to(unit, (8, 128))
    read_index.wait()

    def gather(i):
        k, first = i // 6, i % 6 * (samples // 128 // 6)

        @pl.loop(0, samples // 128 // 6 // group)
        def _(j):
            for t in range(group):
                start = (first + j * group + t) * 128
                both = []
                for h in range(2):
                    block = index[pl.ds(k * rows + 8 * h, 8), pl.ds(aligned(start, 128), 128)]
                    both.append(looked_up(block, table, high * 128).astype(jnp.float32) * scale)
                permuted[k, write_slot, :, pl.ds(aligned(core * samples + start, 128), 128)] = (
                    jnp.concatenate(both, axis=0).astype(jnp.bfloat16)
                )

    def lanes(q):
        return pl.ds(aligned(q * part, 128), part)

    def passed(k, half, from_core):
        q = 2 * from_core + half
        return remote(
            permuted.at[k, 8, :, lanes(q)], permuted.at[k, own_slot, :, lanes(q)],
            pass_send.at[k, half], pass_recv.at[k, half], to_samp=samp ^ 1,
        )

    def pass_on(k, half):
        @pl.when(jnp.logical_not(is_source))
        def _():
            passed(k, half, core).start()

    def moved(axis, by):
        return at(dx=by) if axis == 0 else at(dy=by)

    def sends(k, q, event, slot, directions):
        return [
            remote(
                permuted.at[k, slot, :, lanes(q)], permuted.at[k, slot, :, lanes(q)],
                perm_send.at[k, q, event + i], perm_recv.at[k, q, slot], to_var=moved(axis, by),
            )
            for i, (axis, by) in enumerate(directions)
        ]

    def recv(k, q, slot):
        remote(
            permuted.at[k, slot, :, lanes(q)], permuted.at[k, slot, :, lanes(q)],
            perm_send.at[k, q, 0], perm_recv.at[k, q, slot],
        ).wait_recv()

    def slot_of(dx, dy):
        sx, sy = lax.rem(x - dx + side, side), lax.rem(y - dy + side, side)
        return sx * 2 + lax.rem(sy, 2), sy // 2 == core

    def routes(q):
        return q % 2, (1 if q < 2 else -1)

    def cells(k, q, level):
        axis, way = routes(q)
        other = 1 - axis
        unit_no = 2 * k + q % 2
        straight = unit_no in straight_ring
        both = [(other, way), (other, -way)]
        if unit_no in straight_side:
            both.append((other, 2 * way))
        near, back = way % side, -way % side
        if level == "own":
            ring = [(axis, way), (axis, -way)] + [(axis, 2 * way)] * straight
            found = [(0, 0, 0, ring + both)]
        elif level == "ring":
            found = [(near, 0, 6, [(axis, way)] * (not straight) + both), (back, 0, 10, both)]
        elif level == "far":
            found = [(2, 0, 13, both)]
        elif unit_no in straight_side:
            ends = level == "end"
            found = [(d, s, 0, []) for s in (near, back, 2) for d in range(side) if ends]
        elif level == "side":
            found = [(d, near, 16 + i, [(other, way)]) for i, d in enumerate((0, near, back))]
        elif level == "corner":
            found = [(2, near, 19, [(other, way)])]
        else:
            found = [(d, s, 0, []) for s in (back, 2) for d in range(side)]
        return [(p, s, *rest) if axis == 0 else (s, p, *rest) for p, s, *rest in found]

    def stage(k, q, level, act):
        todo = cells(k, q, level)
        for dy in dict.fromkeys(t[1] for t in todo):

            @pl.when(slot_of(0, dy)[1])
            def _(dy=dy):
                for tx, ty, event, ways in todo:
                    if ty == dy:
                        act(k, q, level, slot_of(tx, ty)[0], event, ways)

    def go(k, q, level, slot, event, ways):
        if level != "own":
            recv(k, q, slot)
        for copy in sends(k, q, event, slot, ways):
            copy.start()

    def done(k, q, level, slot, event, ways):
        for copy in sends(k, q, event, slot, ways):
            copy.wait_send()

    def send_own(k, half):
        for q in range(parts):
            if q % 2 == half:

                @pl.when(jnp.logical_and(is_source, q // 2 == core))
                def _(q=q):
                    stage(k, q, "own", go)

    def send_passed(k, half):
        @pl.when(is_source)
        def _():
            passed(k, half, 1 - core).wait_recv()

        for q in range(parts):
            if q % 2 == half:

                @pl.when(jnp.logical_and(is_source, q // 2 != core))
                def _(q=q):
                    stage(k, q, "own", go)

    def multiply(k, half):
        @pl.loop(0, parts // 2)
        def _(i):
            q = 2 * i + half
            left = permuted[k, pl.ds(0, 8), :, lanes(q)].reshape(8 * rows, part)
            product = jnp.dot(
                left, dose[pl.ds(aligned(q * part, 16), part), :], preferred_element_type=jnp.float32
            )
            tiles = [left[:, 128 * t : 128 * (t + 1)].astype(jnp.float32) for t in range(part // 128)]
            while len(tiles) > 1:
                tiles = [sum(tiles[t : t + 2]) for t in range(0, len(tiles), 2)]
            if half:
                score[k] += product
                row_sum[...] += tiles[0]
            else:

                @pl.when(i == 0)
                def _():
                    score[k] = product
                    row_sum[...] = tiles[0]

                @pl.when(i > 0)
                def _():
                    score[k] += product
                    row_sum[...] += tiles[0]

    def center(k, mean_dose):
        sums = jnp.sum(row_sum[...], axis=1, keepdims=True)
        value = score[k] - sums * mean_dose
        score[k] = value
        leaving[k] = value.astype(jnp.bfloat16)

    def score_copies(k):
        copies = []
        for d in (1, 3, 2):
            to = lax.rem(z + d, side)
            copies.append(
                remote(
                    leaving.at[k, pl.ds(aligned(to * 2 * rows, 2 * rows), 2 * rows)],
                    arrived.at[k, d - 1], score_send.at[k, d - 1], score_recv.at[k, d - 1],
                    to_samp=to * 2 + core,
                )
            )
        return copies

    def inverse_divisor():
        for copy in stat_copies:
            copy.wait_recv()
        sums = jnp.sum(stats[...], axis=0)
        allele_sum, allele_sq = sums[0:1], sums[1:2]
        allele_var = allele_sq / all_samples - (allele_sum / all_samples) ** 2
        inverse = 1.0 / jnp.sqrt(all_samples * (pheno_var + epsilon) * (allele_var + epsilon))
        return inverse, allele_sum / all_samples

    lane = lax.broadcasted_iota(jnp.int32, (2 * rows, 128), 1)

    def local_ends():
        ends = jnp.broadcast_to(marks[...], (8, 128))
        lane8 = lax.broadcasted_iota(jnp.int32, (8, 128), 1)
        offset = 1
        while offset < 128:
            ends = ends + jnp.where(lane8 >= offset, pltpu.roll(ends, offset, axis=1), 0)
            offset *= 2
        return ends - 1 - var * width

    def finish(k, inverse, shared, ends):
        for copy in score_copies(k):
            copy.wait_recv()
        total = score[k, pl.ds(aligned(z * 2 * rows, 2 * rows), 2 * rows), :]
        for d in range(3):
            total = total + arrived[k, d].astype(jnp.float32)
        result = (total + shared) * inverse
        zscore_ref[pl.ds(rows * k, rows), :] = result[:rows]
        zscore_ref[pl.ds(64 + rows * k, rows), :] = result[rows:]
        size = jnp.abs(result)
        best_here = jnp.zeros((2 * rows, 128), jnp.float32)
        for t in range(width // 128):
            run = size[:, 128 * t : 128 * (t + 1)]
            offset = 1
            while offset < 128:
                run = jnp.maximum(run, jnp.where(lane >= offset, pltpu.roll(run, offset, axis=1), 0.0))
                offset *= 2
            here = ends - 128 * t
            source = jnp.minimum(jnp.maximum(here, 0), 127)
            found = jnp.concatenate(
                [
                    jnp.where(
                        here >= 0,
                        jnp.take_along_axis(run[8 * g : 8 * g + 8], source, axis=1, mode="promise_in_bounds"),
                        0.0,
                    )
                    for g in range(2 * rows // 8)
                ],
                axis=0,
            )
            best_here = jnp.maximum(best_here, found)
        best[k] = best_here.astype(jnp.bfloat16)

    def best_copies(k, axis):
        source, target = (best, best_x) if axis == 0 else (best_xy, best_y)
        send, recv_sem = (x_send, x_recv) if axis == 0 else (y_send, y_recv)
        return [
            remote(source.at[k], target.at[k, d - 1], send.at[k, d - 1], recv_sem.at[k, d - 1], to_var=moved(axis, d))
            for d in (1, 3, 2)
        ]

    def join_x(k):
        for copy in best_copies(k, 0):
            copy.wait_recv()
        value = best[k]
        for d in range(3):
            value = jnp.maximum(value, best_x[k, d])
        best_xy[k] = value

    def join_y(k):
        for copy in best_copies(k, 1):
            copy.wait_recv()
        value = best_xy[k]
        for d in range(3):
            value = jnp.maximum(value, best_y[k, d])
        value = value.astype(jnp.float32)
        thresholds_ref[pl.ds(rows * k, rows), :] = value[:rows]
        thresholds_ref[pl.ds(64 + rows * k, rows), :] = value[rows:]

    def start(copies):
        for copy in copies:
            copy.start()

    def wait_dose():
        for i in range(pieces):
            theirs = pl.ds(aligned((1 - core) * samples + i * piece, 16), piece)
            remote(dose.at[theirs], dose.at[theirs], dose_send.at[i], dose_recv.at[i]).wait_recv()

    def drain_passed(k):
        @pl.when(jnp.logical_not(is_source))
        def _():
            for half in range(2):
                passed(k, half, core).wait_send()

    last = chunks - 1
    sent, finished, started = False, [], []
    last_send = [e for e in order if e[0] in ("ring", "far", "side", "corner")][-1]
    for name, *where in order:
        if name == "gather":
            gather(*where)
            if where[0] == 0:
                start([dose_copy(i) for i in range(pieces)] + stat_copies)
            if where[0] == 3:
                read_seg.wait()
                ends = local_ends()
        elif name == "own":
            pass_on(*where)
            send_own(*where)
        elif name == "passed":
            send_passed(*where)
        elif name == "end":
            k, half = where
            for q in range(half, parts, 2):
                stage(k, q, "end", go)
        elif name == "multiply":
            k, half = where
            if k == 0 and half == 0:
                wait_dose()
                inverse, mean_dose = inverse_divisor()
                shared = held_sum * mean_dose
            multiply(k, half)
            if half:
                center(k, mean_dose)
                start(score_copies(k))
        elif name == "finish":
            finish(*where, inverse, shared, ends)
            finished.extend(where)
        else:
            stage(*where, name, go)
        if (name, *where) == last_send:
            sent = True
        while sent and len(started) < len(finished):
            started.append(finished[len(started)])
            start(best_copies(started[-1], 0))
    for k in range(last - 1):
        join_x(k)
        start(best_copies(k, 1))
    finish(last, inverse, shared, ends)
    start(best_copies(last, 0))
    join_x(last - 1)
    start(best_copies(last - 1, 1))
    for copy in trait_copies + stat_copies + [dose_copy(i) for i in range(pieces)]:
        copy.wait_send()
    for k in range(chunks):
        drain_passed(k)
        for q in range(parts):
            for level in ("own", "ring", "far", "side", "corner"):
                stage(k, q, level, done)
        for copy in score_copies(k):
            copy.wait_send()
    join_x(last)
    start(best_copies(last, 1))
    for k in range(chunks):
        join_y(k)
    for k in range(chunks):
        for copy in best_copies(k, 0) + best_copies(k, 1):
            copy.wait_send()


def keep_kernel(zscore_ref, thresholds_ref, zscore_out, thresholds_out, first, second, sem):
    into = [
        pltpu.make_async_copy(zscore_ref, first, sem.at[0]),
        pltpu.make_async_copy(thresholds_ref, second, sem.at[1]),
    ]
    out = [
        pltpu.make_async_copy(first, zscore_out, sem.at[2]),
        pltpu.make_async_copy(second, thresholds_out, sem.at[3]),
    ]
    for copy in into:
        copy.start()
    for copy, after in zip(into, out):
        copy.wait()
        after.start()
    for copy in out:
        copy.wait()


def per_device(dosage, phenotype, perm_index, seg_lengths):
    samples, width = dosage.shape
    segments = seg_lengths.shape[0]
    dma = pltpu.SemaphoreType.DMA
    f32, i32, bf16 = jnp.float32, jnp.int32, jnp.bfloat16
    vmem = pltpu.VMEM
    any_space = pl.BlockSpec(memory_space=pltpu.HBM)
    outs = (
        jax.ShapeDtypeStruct((128, width), f32),
        jax.ShapeDtypeStruct((128, segments), f32),
    )
    zscore, thresholds = pl.pallas_call(
        kernel,
        out_shape=outs,
        in_specs=[any_space] * 4,
        out_specs=(pl.BlockSpec(memory_space=vmem), pl.BlockSpec(memory_space=vmem)),
        scratch_shapes=[
            vmem((8, samples // 128, 128), f32),
            vmem((samples * 4 // 128, 128), i32),
            vmem((samples * 4 // 16, 128), i32),
            vmem(perm_index.shape, i32),
            vmem((samples, width), i32),
            vmem((2 * samples, width), bf16),
            vmem((chunks, 9, rows, 2 * samples), bf16),
            vmem((chunks, 8 * rows, width), f32),
            vmem((8 * rows, 128), f32),
            vmem((chunks, 8 * rows, width), bf16),
            vmem((chunks, 3, 2 * rows, width), bf16),
            vmem((8, 8, width), f32),
            vmem((1, segments), i32),
            vmem((chunks, 2 * rows, segments), bf16),
            vmem((chunks, 3, 2 * rows, segments), bf16),
            vmem((chunks, 2 * rows, segments), bf16),
            vmem((chunks, 3, 2 * rows, segments), bf16),
            dma((3 + pieces,)),
            dma((7,)),
            dma((7,)),
            dma((7,)),
            dma((7,)),
            dma((pieces,)),
            dma((pieces,)),
            dma((chunks, 2)),
            dma((chunks, 2)),
            dma((chunks, parts, 20)),
            dma((chunks, parts, 8)),
            dma((chunks, 3)),
            dma((chunks, 3)),
            dma((chunks, 3)),
            dma((chunks, 3)),
            dma((chunks, 3)),
            dma((chunks, 3)),
        ],
        compiler_params=pltpu.CompilerParams(
            collective_id=0, has_side_effects=True, vmem_limit_bytes=60 * 1024 * 1024
        ),
    )(
        dosage,
        phenotype.reshape(samples // 128, 128),
        perm_index,
        seg_lengths.reshape(1, segments),
    )
    return pl.pallas_call(
        keep_kernel,
        out_shape=outs,
        in_specs=[any_space] * 2,
        out_specs=(any_space, any_space),
        scratch_shapes=[vmem((128, width), f32), vmem((128, segments), f32), dma((4,))],
        compiler_params=pltpu.CompilerParams(vmem_limit_bytes=60 * 1024 * 1024),
    )(zscore, thresholds)


def solution(mesh):
    return jax.shard_map(
        per_device,
        mesh=mesh,
        in_specs=(P("samp", "var"), P("samp"), P("var", "samp"), P()),
        out_specs=(P("samp", "var"), P("samp", None)),
        check_vma=False,
    )
```

```python
import jax
import jax.numpy as jnp
from jax import lax
from jax.experimental import pallas as pl
from jax.experimental.pallas import tpu as pltpu
from jax.sharding import PartitionSpec as P

epsilon = 1e-05
top = 32767.0
side = 4
chunks = 4
rows = 16
parts = 4
pieces = 4
group = 2
MESH = pl.DeviceIdType.MESH

order = [
    ("gather", 0), ("gather", 1), ("gather", 2), ("own", 0, 0), ("gather", 3), ("gather", 4), ("gather", 5),
    ("own", 0, 1), ("passed", 0, 0), ("gather", 6), ("gather", 7), ("passed", 0, 1), ("ring", 0, 0),
    ("gather", 8), ("own", 1, 0), ("gather", 9), ("passed", 1, 0), ("gather", 10), ("ring", 0, 2),
    ("gather", 11), ("ring", 0, 1), ("own", 1, 1), ("passed", 1, 1), ("ring", 0, 3), ("gather", 12),
    ("ring", 1, 0), ("gather", 13), ("ring", 1, 2), ("gather", 14), ("far", 0, 0), ("side", 0, 0),
    ("own", 2, 0), ("gather", 15), ("far", 0, 1), ("passed", 2, 0), ("far", 0, 2), ("side", 0, 2),
    ("gather", 16), ("ring", 1, 3), ("far", 0, 3), ("gather", 17), ("own", 2, 1), ("ring", 1, 1),
    ("far", 1, 0), ("gather", 18), ("passed", 2, 1), ("side", 0, 1), ("ring", 2, 0), ("side", 0, 3),
    ("gather", 19), ("far", 1, 2), ("ring", 2, 2), ("gather", 20), ("corner", 0, 1), ("own", 3, 0),
    ("corner", 0, 3), ("gather", 21), ("side", 1, 2), ("side", 1, 0), ("passed", 3, 0), ("gather", 22),
    ("far", 1, 1), ("ring", 2, 1), ("gather", 23), ("own", 3, 1), ("corner", 0, 0), ("far", 1, 3),
    ("ring", 2, 3), ("passed", 3, 1), ("far", 2, 0), ("end", 0, 1), ("side", 1, 1), ("side", 1, 3),
    ("corner", 0, 2), ("corner", 1, 1), ("far", 2, 1), ("corner", 1, 0), ("far", 2, 2), ("far", 2, 3),
    ("ring", 3, 0), ("corner", 1, 2), ("ring", 3, 2), ("corner", 1, 3), ("ring", 3, 1), ("ring", 3, 3),
    ("side", 2, 0), ("side", 2, 2), ("side", 2, 3), ("corner", 2, 2), ("corner", 2, 0), ("end", 0, 0),
    ("multiply", 0, 0), ("side", 2, 1), ("multiply", 0, 1), ("far", 3, 0), ("far", 3, 1), ("far", 3, 2),
    ("side", 3, 0), ("corner", 2, 1), ("far", 3, 3), ("end", 1, 1), ("corner", 2, 3), ("end", 1, 0),
    ("side", 3, 2), ("multiply", 1, 0), ("multiply", 1, 1), ("side", 3, 1), ("end", 2, 0), ("corner", 3, 2),
    ("corner", 3, 0), ("side", 3, 3), ("multiply", 2, 0), ("corner", 3, 1), ("corner", 3, 3), ("end", 2, 1),
    ("multiply", 2, 1), ("finish", 0), ("finish", 1), ("end", 3, 0), ("multiply", 3, 0), ("end", 3, 1),
    ("multiply", 3, 1), ("finish", 2),
]


def looked_up(index, table_ref, half_at):
    high_half = index >= half_at
    word = jnp.where(high_half, index - half_at, index)
    lane = lax.bitwise_and(word, 127)
    row = lax.shift_right_logical(word, 7)
    count = half_at // 128
    levels = max(1, (count - 1).bit_length())
    bits = [lax.bitwise_and(row, 1 << k) != 0 for k in range(levels)]

    def pick(level, base):
        if level == 0:
            source = table_ref[pl.ds(base * 8, 8), :]
            return jnp.take_along_axis(source, lane, axis=1, mode="promise_in_bounds")
        low = pick(level - 1, base)
        if base + (1 << (level - 1)) >= count:
            return low
        high = pick(level - 1, base + (1 << (level - 1)))
        return jnp.where(bits[level - 1], high, low)

    words = pick(levels, 0)
    low_part = lax.shift_right_arithmetic(lax.shift_left(words, 16), 16)
    return jnp.where(high_half, lax.shift_right_arithmetic(words, 16), low_part)


def aligned(value, by):
    return pl.multiple_of(value, by)


def kernel(
    dosage_ref, pheno_ref, index_ref, seg_ref, zscore_out, thresholds_out, zscore_ref, thresholds_ref,
    traits, words, table, index, counts, dose, permuted, score, row_sum, leaving, arrived, stats, marks,
    best, best_x, best_xy, best_y,
    local_sem, trait_send, trait_recv, stat_recv, dose_send, dose_recv,
    pass_send, pass_recv, perm_send, perm_recv, score_send, score_recv,
    x_send, x_recv, y_send, y_recv,
):
    samples, width = dosage_ref.shape
    var, samp = lax.axis_index("var"), lax.axis_index("samp")
    x, y = var // side, var % side
    z, core = samp // 2, samp % 2
    all_samples = 8 * samples
    part = 2 * samples // parts
    is_source = y // 2 == core
    own_slot = x * 2 + y % 2
    write_slot = jnp.where(is_source, own_slot, 8)

    def at(dx=0, dy=0):
        return lax.rem(x + dx + side, side) * side + lax.rem(y + dy + side, side)

    def remote(src, dst, send, recv, to_var=None, to_samp=None):
        return pltpu.make_async_remote_copy(
            src_ref=src, dst_ref=dst, send_sem=send, recv_sem=recv,
            device_id={
                "var": var if to_var is None else to_var,
                "samp": samp if to_samp is None else to_samp,
            },
            device_id_type=MESH,
        )

    piece = samples // pieces
    read_pheno = pltpu.make_async_copy(pheno_ref, traits.at[samp], local_sem.at[0])
    read_index = pltpu.make_async_copy(index_ref, index, local_sem.at[1])
    read_seg = pltpu.make_async_copy(seg_ref, marks, local_sem.at[2])
    read_dose = [
        pltpu.make_async_copy(
            dosage_ref.at[pl.ds(i * piece, piece)], counts.at[pl.ds(i * piece, piece)],
            local_sem.at[3 + i],
        )
        for i in range(pieces)
    ]
    read_pheno.start()
    for copy in read_dose[:2]:
        copy.start()
    read_index.start()
    read_seg.start()
    for copy in read_dose[2:]:
        copy.start()

    barrier = pltpu.get_barrier_semaphore()
    samp_peers = [lax.rem(samp + d, 8) for d in range(1, 8)]
    for peer in samp_peers:
        pl.semaphore_signal(barrier, inc=1, device_id={"var": var, "samp": peer}, device_id_type=MESH)
    for d in range(1, side):
        for to in (at(dx=d), at(dy=d)):
            pl.semaphore_signal(barrier, inc=1, device_id={"var": to, "samp": samp}, device_id_type=MESH)
    trait_copies = [
        remote(traits.at[samp], traits.at[samp], trait_send.at[d], trait_recv.at[d], to_samp=samp_peers[d])
        for d in range(7)
    ]

    def dose_copy(of_core):
        at_rows = pl.ds(aligned(of_core * samples, 16), samples)
        return remote(dose.at[at_rows], dose.at[at_rows], dose_send.at[0], dose_recv.at[0], to_samp=samp ^ 1)

    def convert(i):
        read_dose[i].wait()
        step = 32

        def body(r, sums):
            one, two = sums
            for h in range(step // 16):
                start = i * piece + r * step + 16 * h
                value = counts[pl.ds(aligned(start, 16), 16), :].astype(jnp.float32)
                dose[pl.ds(aligned(core * samples + start, 16), 16), :] = value.astype(jnp.bfloat16)
                one = one + (value[:8] + value[8:])
                two = two + (value[:8] * value[:8] + value[8:] * value[8:])
            return one, two

        zero = jnp.zeros((8, width), jnp.float32)
        one, two = lax.fori_loop(0, piece // step, body, (zero, zero))
        if i == 0:
            stats[samp] = jnp.zeros((8, width), jnp.float32)
        stats[samp, 0:1, :] += jnp.sum(one, axis=0, keepdims=True)
        stats[samp, 1:2, :] += jnp.sum(two, axis=0, keepdims=True)

    stat_copies = [
        remote(stats.at[samp], stats.at[samp], trait_send.at[d], stat_recv.at[d], to_samp=samp_peers[d])
        for d in range(7)
    ]

    for i in range(pieces):
        convert(i)
    read_pheno.wait()
    pl.semaphore_wait(barrier, 13)
    for copy in trait_copies:
        copy.start()

    for copy in trait_copies:
        copy.wait_recv()
    high = all_samples // 2 // 128

    values = traits[...].reshape(2 * high, 128)
    mean = jnp.sum(jnp.sum(values, axis=0, keepdims=True), axis=1, keepdims=True) / all_samples
    centered = values - mean
    square = jnp.sum(centered * centered, axis=0, keepdims=True)
    pheno_var = jnp.sum(square, axis=1, keepdims=True) / all_samples
    largest = jnp.max(jnp.max(jnp.abs(centered), axis=0, keepdims=True), axis=1, keepdims=True)
    unit = jnp.where(largest > 0, largest / top, 1.0)
    fixed = jnp.round(centered / unit).astype(jnp.int32)
    words[...] = jnp.bitwise_or(
        jnp.bitwise_and(fixed[:high], 65535), lax.shift_left(fixed[high:], 16)
    )
    for r in range(high):
        table[pl.ds(8 * r, 8), :] = jnp.broadcast_to(words[pl.ds(r, 1), :], (8, 128))
    held = (fixed.astype(jnp.float32) * unit).astype(jnp.bfloat16).astype(jnp.float32)
    held_sum = jnp.sum(jnp.sum(held, axis=0, keepdims=True), axis=1, keepdims=True)
    scale = jnp.broadcast_to(unit, (8, 128))
    read_index.wait()

    def gather(i):
        k, first = i // 6, i % 6 * (samples // 128 // 6)

        @pl.loop(0, samples // 128 // 6 // group)
        def _(j):
            for t in range(group):
                start = (first + j * group + t) * 128
                both = []
                for h in range(2):
                    block = index[pl.ds(k * rows + 8 * h, 8), pl.ds(aligned(start, 128), 128)]
                    both.append(looked_up(block, table, high * 128).astype(jnp.float32) * scale)
                permuted[k, write_slot, :, pl.ds(aligned(core * samples + start, 128), 128)] = (
                    jnp.concatenate(both, axis=0).astype(jnp.bfloat16)
                )

    def lanes(q):
        return pl.ds(aligned(q * part, 128), part)

    def passed(k, half, from_core):
        q = 2 * from_core + half
        return remote(
            permuted.at[k, 8, :, lanes(q)], permuted.at[k, own_slot, :, lanes(q)],
            pass_send.at[half], pass_recv.at[k, half], to_samp=samp ^ 1,
        )

    def pass_on(k, half):
        @pl.when(jnp.logical_not(is_source))
        def _():
            if k:
                passed(k - 1, half, core).wait_send()
            passed(k, half, core).start()

    def moved(axis, by):
        return at(dx=by) if axis == 0 else at(dy=by)

    def sends(k, q, event, slot, directions):
        return [
            remote(
                permuted.at[k, slot, :, lanes(q)], permuted.at[k, slot, :, lanes(q)],
                perm_send.at[q, event + i], perm_recv.at[k, q, slot], to_var=moved(axis, by),
            )
            for i, (axis, by) in enumerate(directions)
        ]

    def recv(k, q, slot):
        remote(
            permuted.at[k, slot, :, lanes(q)], permuted.at[k, slot, :, lanes(q)],
            perm_send.at[q, 0], perm_recv.at[k, q, slot],
        ).wait_recv()

    def slot_of(dx, dy):
        sx, sy = lax.rem(x - dx + side, side), lax.rem(y - dy + side, side)
        return sx * 2 + lax.rem(sy, 2), sy // 2 == core

    def routes(q):
        return q % 2, (1 if q < 2 else -1)

    def cells(q, level):
        axis, way = routes(q)
        other = 1 - axis
        both = [(other, way), (other, -way)]
        near, back = way % side, -way % side
        if level == "own":
            found = [(0, 0, 0, [(axis, way), (axis, -way), *both])]
        elif level == "ring":
            found = [(near, 0, 4, [(axis, way), *both]), (back, 0, 7, both)]
        elif level == "far":
            found = [(2, 0, 9, both)]
        elif level == "side":
            found = [(d, near, 11 + i, [(other, way)]) for i, d in enumerate((0, near, back))]
        elif level == "corner":
            found = [(2, near, 14, [(other, way)])]
        else:
            found = [(d, s, 0, []) for s in (back, 2) for d in range(side)]
        return [(p, s, *rest) if axis == 0 else (s, p, *rest) for p, s, *rest in found]

    def stage(k, q, level, act):
        todo = cells(q, level)
        for dy in dict.fromkeys(t[1] for t in todo):

            @pl.when(slot_of(0, dy)[1])
            def _(dy=dy):
                for tx, ty, event, ways in todo:
                    if ty == dy:
                        act(k, q, level, slot_of(tx, ty)[0], event, ways)

    def go(k, q, level, slot, event, ways):
        if level != "own":
            recv(k, q, slot)
        earlier = before.get((q, level)) if level != "own" else (k - 1 if k else None)
        if ways and earlier is not None:
            done(earlier, q, level, slot, event, ways)
        for copy in sends(k, q, event, slot, ways):
            copy.start()

    def done(k, q, level, slot, event, ways):
        for copy in sends(k, q, event, slot, ways):
            copy.wait_send()

    before = {}

    def step(k, q, level):
        stage(k, q, level, go)
        before[q, level] = k

    def send_own(k, half):
        for q in range(parts):
            if q % 2 == half:

                @pl.when(jnp.logical_and(is_source, q // 2 == core))
                def _(q=q):
                    stage(k, q, "own", go)

    def send_passed(k, half):
        @pl.when(is_source)
        def _():
            passed(k, half, 1 - core).wait_recv()

        for q in range(parts):
            if q % 2 == half:

                @pl.when(jnp.logical_and(is_source, q // 2 != core))
                def _(q=q):
                    stage(k, q, "own", go)

    def multiply(k, half):
        @pl.loop(0, parts // 2)
        def _(i):
            q = 2 * i + half
            left = permuted[k, pl.ds(0, 8), :, lanes(q)].reshape(8 * rows, part)
            product = jnp.dot(
                left, dose[pl.ds(aligned(q * part, 16), part), :], preferred_element_type=jnp.float32
            )
            tiles = [left[:, 128 * t : 128 * (t + 1)].astype(jnp.float32) for t in range(part // 128)]
            while len(tiles) > 1:
                tiles = [sum(tiles[t : t + 2]) for t in range(0, len(tiles), 2)]
            if half:
                score[k] += product
                row_sum[...] += tiles[0]
            else:

                @pl.when(i == 0)
                def _():
                    score[k] = product
                    row_sum[...] = tiles[0]

                @pl.when(i > 0)
                def _():
                    score[k] += product
                    row_sum[...] += tiles[0]

    def center(k, mean_dose):
        sums = jnp.sum(row_sum[...], axis=1, keepdims=True)
        value = score[k] - sums * mean_dose
        score[k] = value
        leaving[k] = value.astype(jnp.bfloat16)

    def score_copies(k):
        copies = []
        for d in (1, 3, 2):
            to = lax.rem(z + d, side)
            copies.append(
                remote(
                    leaving.at[k, pl.ds(aligned(to * 2 * rows, 2 * rows), 2 * rows)],
                    arrived.at[k, d - 1], score_send.at[d - 1], score_recv.at[k, d - 1],
                    to_samp=to * 2 + core,
                )
            )
        return copies

    def inverse_divisor():
        for copy in stat_copies:
            copy.wait_recv()
        sums = jnp.sum(stats[...], axis=0)
        allele_sum, allele_sq = sums[0:1], sums[1:2]
        allele_var = allele_sq / all_samples - (allele_sum / all_samples) ** 2
        inverse = 1.0 / jnp.sqrt(all_samples * (pheno_var + epsilon) * (allele_var + epsilon))
        return inverse, allele_sum / all_samples

    lane = lax.broadcasted_iota(jnp.int32, (2 * rows, 128), 1)

    def local_ends():
        ends = jnp.broadcast_to(marks[...], (8, 128))
        lane8 = lax.broadcasted_iota(jnp.int32, (8, 128), 1)
        offset = 1
        while offset < 128:
            ends = ends + jnp.where(lane8 >= offset, pltpu.roll(ends, offset, axis=1), 0)
            offset *= 2
        return ends - 1 - var * width

    def finish(k, inverse, shared, ends):
        for copy in score_copies(k):
            copy.wait_recv()
        total = score[k, pl.ds(aligned(z * 2 * rows, 2 * rows), 2 * rows), :]
        for d in range(3):
            total = total + arrived[k, d].astype(jnp.float32)
        result = (total + shared) * inverse
        zscore_ref[pl.ds(rows * k, rows), :] = result[:rows]
        zscore_ref[pl.ds(64 + rows * k, rows), :] = result[rows:]
        size = jnp.abs(result)
        best_here = jnp.zeros((2 * rows, 128), jnp.float32)
        for t in range(width // 128):
            run = size[:, 128 * t : 128 * (t + 1)]
            offset = 1
            while offset < 128:
                run = jnp.maximum(run, jnp.where(lane >= offset, pltpu.roll(run, offset, axis=1), 0.0))
                offset *= 2
            here = ends - 128 * t
            source = jnp.minimum(jnp.maximum(here, 0), 127)
            found = jnp.concatenate(
                [
                    jnp.where(
                        here >= 0,
                        jnp.take_along_axis(run[8 * g : 8 * g + 8], source, axis=1, mode="promise_in_bounds"),
                        0.0,
                    )
                    for g in range(2 * rows // 8)
                ],
                axis=0,
            )
            best_here = jnp.maximum(best_here, found)
        best[k] = best_here.astype(jnp.bfloat16)

    def best_copies(k, axis):
        source, target = (best, best_x) if axis == 0 else (best_xy, best_y)
        send, recv_sem = (x_send, x_recv) if axis == 0 else (y_send, y_recv)
        return [
            remote(source.at[k], target.at[k, d - 1], send.at[d - 1], recv_sem.at[k, d - 1], to_var=moved(axis, d))
            for d in (1, 3, 2)
        ]

    def join_x(k):
        for copy in best_copies(k, 0):
            copy.wait_recv()
        value = best[k]
        for d in range(3):
            value = jnp.maximum(value, best_x[k, d])
        best_xy[k] = value

    def join_y(k):
        for copy in best_copies(k, 1):
            copy.wait_recv()
        value = best_xy[k]
        for d in range(3):
            value = jnp.maximum(value, best_y[k, d])
        value = value.astype(jnp.float32)
        thresholds_ref[pl.ds(rows * k, rows), :] = value[:rows]
        thresholds_ref[pl.ds(64 + rows * k, rows), :] = value[rows:]

    def sent_all(copies):
        for copy in copies:
            copy.wait_send()

    def send_best(k, axis):
        if k:
            sent_all(best_copies(k - 1, axis))
        start(best_copies(k, axis))

    def start(copies):
        for copy in copies:
            copy.start()

    def wait_dose():
        dose_copy(1 - core).wait_recv()

    def drain_passed(k):
        @pl.when(jnp.logical_not(is_source))
        def _():
            for half in range(2):
                passed(k, half, core).wait_send()

    last = chunks - 1
    sent, finished, started = False, [], []
    last_send = [e for e in order if e[0] in ("ring", "far", "side", "corner")][-1]
    for name, *where in order:
        if name == "gather":
            gather(*where)
            if where[0] == 0:
                sent_all(trait_copies)
                start([dose_copy(core)] + stat_copies)
            if where[0] == 3:
                read_seg.wait()
                ends = local_ends()
        elif name == "own":
            pass_on(*where)
            send_own(*where)
        elif name == "passed":
            send_passed(*where)
        elif name == "end":
            k, half = where
            for q in range(half, parts, 2):
                stage(k, q, "end", go)
        elif name == "multiply":
            k, half = where
            if k == 0 and half == 0:
                wait_dose()
                inverse, mean_dose = inverse_divisor()
                shared = held_sum * mean_dose
            multiply(k, half)
            if half:
                center(k, mean_dose)
                if k:
                    sent_all(score_copies(k - 1))
                start(score_copies(k))
        elif name == "finish":
            finish(*where, inverse, shared, ends)
            finished.extend(where)
        else:
            step(*where, name)
        if (name, *where) == last_send:
            sent = True
        while sent and len(started) < len(finished):
            started.append(finished[len(started)])
            send_best(started[-1], 0)
    for k in range(last - 1):
        join_x(k)
        send_best(k, 1)
    finish(last, inverse, shared, ends)
    keep_zscore = pltpu.make_async_copy(zscore_ref, zscore_out, local_sem.at[0])
    keep_zscore.start()
    send_best(last, 0)
    join_x(last - 1)
    send_best(last - 1, 1)
    sent_all(stat_copies + [dose_copy(core)])
    drain_passed(last)
    for q in range(parts):
        stage(last, q, "own", done)
        for level in ("ring", "far", "side", "corner"):
            stage(before[q, level], q, level, done)
    sent_all(score_copies(last))
    for k in range(last - 1):
        join_y(k)
    join_x(last)
    send_best(last, 1)
    join_y(last - 1)
    sent_all(best_copies(last, 0))
    join_y(last)
    keep = pltpu.make_async_copy(thresholds_ref, thresholds_out, local_sem.at[1])
    keep.start()
    sent_all(best_copies(last, 1))
    keep_zscore.wait()
    keep.wait()


def keep_kernel(zscore_ref, thresholds_ref, zscore_out, thresholds_out, first, second, sem):
    into = [
        pltpu.make_async_copy(zscore_ref, first, sem.at[0]),
        pltpu.make_async_copy(thresholds_ref, second, sem.at[1]),
    ]
    out = [
        pltpu.make_async_copy(first, zscore_out, sem.at[2]),
        pltpu.make_async_copy(second, thresholds_out, sem.at[3]),
    ]
    for copy in into:
        copy.start()
    for copy, after in zip(into, out):
        copy.wait()
        after.start()
    for copy in out:
        copy.wait()


def per_device(dosage, phenotype, perm_index, seg_lengths):
    samples, width = dosage.shape
    segments = seg_lengths.shape[0]
    dma = pltpu.SemaphoreType.DMA
    f32, i32, bf16 = jnp.float32, jnp.int32, jnp.bfloat16
    vmem = pltpu.VMEM
    any_space = pl.BlockSpec(memory_space=pltpu.HBM)
    outs = (
        jax.ShapeDtypeStruct((128, width), f32),
        jax.ShapeDtypeStruct((128, segments), f32),
    )
    zscore, thresholds = pl.pallas_call(
        kernel,
        out_shape=outs,
        in_specs=[any_space] * 4,
        out_specs=(any_space, any_space),
        scratch_shapes=[
            vmem((128, width), f32),
            vmem((128, segments), f32),
            vmem((8, samples // 128, 128), f32),
            vmem((samples * 4 // 128, 128), i32),
            vmem((samples * 4 // 16, 128), i32),
            vmem(perm_index.shape, i32),
            vmem((samples, width), i32),
            vmem((2 * samples, width), bf16),
            vmem((chunks, 9, rows, 2 * samples), bf16),
            vmem((chunks, 8 * rows, width), f32),
            vmem((8 * rows, 128), f32),
            vmem((chunks, 8 * rows, width), bf16),
            vmem((chunks, 3, 2 * rows, width), bf16),
            vmem((8, 8, width), f32),
            vmem((1, segments), i32),
            vmem((chunks, 2 * rows, segments), bf16),
            vmem((chunks, 3, 2 * rows, segments), bf16),
            vmem((chunks, 2 * rows, segments), bf16),
            vmem((chunks, 3, 2 * rows, segments), bf16),
            dma((3 + pieces,)),
            dma((7,)),
            dma((7,)),
            dma((7,)),
            dma((1,)),
            dma((1,)),
            dma((2,)),
            dma((chunks, 2)),
            dma((parts, 15)),
            dma((chunks, parts, 8)),
            dma((3,)),
            dma((chunks, 3)),
            dma((3,)),
            dma((chunks, 3)),
            dma((3,)),
            dma((chunks, 3)),
        ],
        compiler_params=pltpu.CompilerParams(
            collective_id=0, has_side_effects=True, vmem_limit_bytes=60 * 1024 * 1024
        ),
    )(
        dosage,
        phenotype.reshape(samples // 128, 128),
        perm_index,
        seg_lengths.reshape(1, segments),
    )
    return pl.pallas_call(
        keep_kernel,
        out_shape=outs,
        in_specs=[any_space] * 2,
        out_specs=(any_space, any_space),
        scratch_shapes=[vmem((128, width), f32), vmem((128, segments), f32), dma((4,))],
        compiler_params=pltpu.CompilerParams(vmem_limit_bytes=60 * 1024 * 1024),
    )(zscore, thresholds)


def solution(mesh):
    return jax.shard_map(
        per_device,
        mesh=mesh,
        in_specs=(P("samp", "var"), P("samp"), P("var", "samp"), P()),
        out_specs=(P("samp", "var"), P("samp", None)),
        check_vma=False,
    )
```

```python
import jax
import jax.numpy as jnp
from jax import lax
from jax.experimental import pallas as pl
from jax.experimental.pallas import tpu as pltpu
from jax.sharding import PartitionSpec as P

epsilon = 1e-05
top = 32767.0
side = 4
chunks = 4
rows = 16
parts = 4
pieces = 4
group = 2
MESH = pl.DeviceIdType.MESH

order = [
    ("gather", 0), ("gather", 1), ("gather", 2), ("own", 0, 0), ("gather", 3), ("gather", 4),
    ("passed", 0, 0), ("gather", 5), ("own", 0, 1), ("gather", 6), ("gather", 7), ("ring", 0, 0),
    ("passed", 0, 1), ("gather", 8), ("own", 1, 0), ("gather", 9), ("passed", 1, 0), ("ring", 0, 2),
    ("gather", 10), ("ring", 0, 1), ("gather", 11), ("own", 1, 1), ("far", 0, 0), ("gather", 12),
    ("passed", 1, 1), ("ring", 1, 0), ("gather", 13), ("ring", 0, 3), ("ring", 1, 2), ("side", 0, 0),
    ("far", 0, 2), ("gather", 14), ("own", 2, 0), ("gather", 15), ("side", 0, 1), ("side", 0, 2),
    ("passed", 2, 0), ("gather", 16), ("far", 0, 1), ("gather", 17), ("own", 2, 1), ("passed", 2, 1),
    ("ring", 1, 1), ("side", 0, 3), ("gather", 18), ("ring", 1, 3), ("ring", 2, 0), ("far", 1, 2),
    ("far", 1, 0), ("gather", 19), ("far", 0, 3), ("gather", 20), ("own", 3, 0), ("corner", 0, 0),
    ("ring", 2, 2), ("corner", 0, 2), ("passed", 3, 0), ("gather", 21), ("corner", 0, 1), ("gather", 22),
    ("ring", 2, 1), ("ring", 2, 3), ("gather", 23), ("own", 3, 1), ("far", 1, 1), ("passed", 3, 1),
    ("far", 1, 3), ("end", 0, 0), ("corner", 0, 3), ("far", 2, 0), ("far", 2, 1), ("ring", 3, 0),
    ("side", 1, 1), ("side", 1, 2), ("side", 1, 0), ("ring", 3, 2), ("far", 2, 3), ("multiply", 0, 0),
    ("ring", 3, 1), ("side", 1, 3), ("ring", 3, 3), ("corner", 1, 0), ("far", 2, 2), ("corner", 1, 3),
    ("corner", 1, 2), ("far", 3, 0), ("end", 0, 1), ("corner", 1, 1), ("side", 2, 0), ("corner", 2, 0),
    ("far", 3, 2), ("side", 2, 1), ("multiply", 0, 1), ("side", 2, 2), ("far", 3, 3), ("side", 2, 3),
    ("corner", 2, 3), ("far", 3, 1), ("corner", 2, 1), ("side", 3, 0), ("corner", 2, 2), ("side", 3, 2),
    ("end", 1, 0), ("multiply", 1, 0), ("corner", 3, 0), ("end", 1, 1), ("corner", 3, 2), ("side", 3, 3),
    ("multiply", 1, 1), ("side", 3, 1), ("end", 2, 0), ("corner", 3, 1), ("corner", 3, 3), ("multiply", 2, 0),
    ("end", 2, 1), ("multiply", 2, 1), ("finish", 0), ("end", 3, 0), ("multiply", 3, 0), ("finish", 1),
    ("end", 3, 1), ("multiply", 3, 1), ("finish", 2),
]


def looked_up(index, table_ref, half_at):
    high_half = index >= half_at
    word = jnp.where(high_half, index - half_at, index)
    lane = lax.bitwise_and(word, 127)
    row = lax.shift_right_logical(word, 7)
    count = half_at // 128
    levels = max(1, (count - 1).bit_length())
    bits = [lax.bitwise_and(row, 1 << k) != 0 for k in range(levels)]

    def pick(level, base):
        if level == 0:
            source = table_ref[pl.ds(base * 8, 8), :]
            return jnp.take_along_axis(source, lane, axis=1, mode="promise_in_bounds")
        low = pick(level - 1, base)
        if base + (1 << (level - 1)) >= count:
            return low
        high = pick(level - 1, base + (1 << (level - 1)))
        return jnp.where(bits[level - 1], high, low)

    words = pick(levels, 0)
    low_part = lax.shift_right_arithmetic(lax.shift_left(words, 16), 16)
    return jnp.where(high_half, lax.shift_right_arithmetic(words, 16), low_part)


def aligned(value, by):
    return pl.multiple_of(value, by)


def kernel(
    dosage_ref, pheno_ref, index_ref, seg_ref, zscore_out, thresholds_out, zscore_ref, thresholds_ref,
    traits, words, table, index, counts, dose, permuted, score, row_sum, leaving, arrived, stats, marks,
    best, best_x, best_xy, best_y,
    local_sem, trait_send, trait_recv, stat_recv, dose_send, dose_recv,
    pass_send, pass_recv, perm_send, perm_recv, score_send, score_recv,
    x_send, x_recv, y_send, y_recv,
):
    samples, width = dosage_ref.shape
    var, samp = lax.axis_index("var"), lax.axis_index("samp")
    x, y = var // side, var % side
    z, core = samp // 2, samp % 2
    all_samples = 8 * samples
    part = 2 * samples // parts
    is_source = y // 2 == core
    own_slot = x * 2 + y % 2
    write_slot = jnp.where(is_source, own_slot, 8)

    def at(dx=0, dy=0):
        return lax.rem(x + dx + side, side) * side + lax.rem(y + dy + side, side)

    def remote(src, dst, send, recv, to_var=None, to_samp=None):
        return pltpu.make_async_remote_copy(
            src_ref=src, dst_ref=dst, send_sem=send, recv_sem=recv,
            device_id={
                "var": var if to_var is None else to_var,
                "samp": samp if to_samp is None else to_samp,
            },
            device_id_type=MESH,
        )

    piece = samples // pieces
    read_pheno = pltpu.make_async_copy(pheno_ref, traits.at[samp], local_sem.at[0])
    read_index = pltpu.make_async_copy(index_ref, index, local_sem.at[1])
    read_seg = pltpu.make_async_copy(seg_ref, marks, local_sem.at[2])
    read_dose = [
        pltpu.make_async_copy(
            dosage_ref.at[pl.ds(i * piece, piece)], counts.at[pl.ds(i * piece, piece)],
            local_sem.at[3 + i],
        )
        for i in range(pieces)
    ]
    read_pheno.start()
    for copy in read_dose[:2]:
        copy.start()
    read_index.start()
    read_seg.start()
    for copy in read_dose[2:]:
        copy.start()

    barrier = pltpu.get_barrier_semaphore()
    samp_peers = [lax.rem(samp + d, 8) for d in range(1, 8)]
    for peer in samp_peers:
        pl.semaphore_signal(barrier, inc=1, device_id={"var": var, "samp": peer}, device_id_type=MESH)
    for d in range(1, side):
        for to in (at(dx=d), at(dy=d)):
            pl.semaphore_signal(barrier, inc=1, device_id={"var": to, "samp": samp}, device_id_type=MESH)
    trait_copies = [
        remote(traits.at[samp], traits.at[samp], trait_send.at[d], trait_recv.at[d], to_samp=samp_peers[d])
        for d in range(7)
    ]

    def dose_copy(of_core):
        at_rows = pl.ds(aligned(of_core * samples, 16), samples)
        return remote(dose.at[at_rows], dose.at[at_rows], dose_send.at[0], dose_recv.at[0], to_samp=samp ^ 1)

    def convert(i):
        read_dose[i].wait()
        step = 32

        def body(r, sums):
            one, two = sums
            for h in range(step // 16):
                start = i * piece + r * step + 16 * h
                value = counts[pl.ds(aligned(start, 16), 16), :].astype(jnp.float32)
                dose[pl.ds(aligned(core * samples + start, 16), 16), :] = value.astype(jnp.bfloat16)
                one = one + (value[:8] + value[8:])
                two = two + (value[:8] * value[:8] + value[8:] * value[8:])
            return one, two

        zero = jnp.zeros((8, width), jnp.float32)
        one, two = lax.fori_loop(0, piece // step, body, (zero, zero))
        if i == 0:
            stats[samp] = jnp.zeros((8, width), jnp.float32)
        stats[samp, 0:1, :] += jnp.sum(one, axis=0, keepdims=True)
        stats[samp, 1:2, :] += jnp.sum(two, axis=0, keepdims=True)

    stat_copies = [
        remote(stats.at[samp], stats.at[samp], trait_send.at[d], stat_recv.at[d], to_samp=samp_peers[d])
        for d in range(7)
    ]

    for i in range(pieces):
        convert(i)
    read_pheno.wait()
    pl.semaphore_wait(barrier, 13)
    for copy in trait_copies:
        copy.start()

    for copy in trait_copies:
        copy.wait_recv()
    high = all_samples // 2 // 128

    values = traits[...].reshape(2 * high, 128)
    mean = jnp.sum(jnp.sum(values, axis=0, keepdims=True), axis=1, keepdims=True) / all_samples
    centered = values - mean
    square = jnp.sum(centered * centered, axis=0, keepdims=True)
    pheno_var = jnp.sum(square, axis=1, keepdims=True) / all_samples
    largest = jnp.max(jnp.max(jnp.abs(centered), axis=0, keepdims=True), axis=1, keepdims=True)
    unit = jnp.where(largest > 0, largest / top, 1.0)
    fixed = jnp.round(centered / unit).astype(jnp.int32)
    words[...] = jnp.bitwise_or(
        jnp.bitwise_and(fixed[:high], 65535), lax.shift_left(fixed[high:], 16)
    )
    for r in range(high):
        table[pl.ds(8 * r, 8), :] = jnp.broadcast_to(words[pl.ds(r, 1), :], (8, 128))
    held = (fixed.astype(jnp.float32) * unit).astype(jnp.bfloat16).astype(jnp.float32)
    held_sum = jnp.sum(jnp.sum(held, axis=0, keepdims=True), axis=1, keepdims=True)
    scale = jnp.broadcast_to(unit, (8, 128))
    read_index.wait()

    def gather(i):
        k, first = i // 6, i % 6 * (samples // 128 // 6)

        @pl.loop(0, samples // 128 // 6 // group)
        def _(j):
            for t in range(group):
                start = (first + j * group + t) * 128
                both = []
                for h in range(2):
                    block = index[pl.ds(k * rows + 8 * h, 8), pl.ds(aligned(start, 128), 128)]
                    both.append(looked_up(block, table, high * 128).astype(jnp.float32) * scale)
                permuted[k, write_slot, :, pl.ds(aligned(core * samples + start, 128), 128)] = (
                    jnp.concatenate(both, axis=0).astype(jnp.bfloat16)
                )

    def lanes(q):
        return pl.ds(aligned(q * part, 128), part)

    def passed(k, half, from_core):
        q = 2 * from_core + half
        return remote(
            permuted.at[k, 8, :, lanes(q)], permuted.at[k, own_slot, :, lanes(q)],
            pass_send.at[half], pass_recv.at[k, half], to_samp=samp ^ 1,
        )

    def pass_on(k, half):
        @pl.when(jnp.logical_not(is_source))
        def _():
            if k:
                passed(k - 1, half, core).wait_send()
            passed(k, half, core).start()

    def moved(axis, by):
        return at(dx=by) if axis == 0 else at(dy=by)

    def sends(k, q, event, slot, directions):
        return [
            remote(
                permuted.at[k, slot, :, lanes(q)], permuted.at[k, slot, :, lanes(q)],
                perm_send.at[q, event + i], perm_recv.at[k, q, slot], to_var=moved(axis, by),
            )
            for i, (axis, by) in enumerate(directions)
        ]

    def recv(k, q, slot):
        remote(
            permuted.at[k, slot, :, lanes(q)], permuted.at[k, slot, :, lanes(q)],
            perm_send.at[q, 0], perm_recv.at[k, q, slot],
        ).wait_recv()

    def slot_of(dx, dy):
        sx, sy = lax.rem(x - dx + side, side), lax.rem(y - dy + side, side)
        return sx * 2 + lax.rem(sy, 2), sy // 2 == core

    def routes(q):
        return q % 2, (1 if q < 2 else -1)

    def cells(q, level):
        axis, way = routes(q)
        other = 1 - axis
        both = [(other, way), (other, -way)]
        near, back = way % side, -way % side
        if level == "own":
            found = [(0, 0, 0, [(axis, way), (axis, -way), *both])]
        elif level == "ring":
            found = [(near, 0, 4, [(axis, way), *both]), (back, 0, 7, both)]
        elif level == "far":
            found = [(2, 0, 9, both)]
        elif level == "side":
            found = [(d, near, 11 + i, [(other, way)]) for i, d in enumerate((0, near, back))]
        elif level == "corner":
            found = [(2, near, 14, [(other, way)])]
        else:
            found = [(d, s, 0, []) for s in (back, 2) for d in range(side)]
        return [(p, s, *rest) if axis == 0 else (s, p, *rest) for p, s, *rest in found]

    def stage(k, q, level, act):
        todo = cells(q, level)
        for dy in dict.fromkeys(t[1] for t in todo):

            @pl.when(slot_of(0, dy)[1])
            def _(dy=dy):
                for tx, ty, event, ways in todo:
                    if ty == dy:
                        act(k, q, level, slot_of(tx, ty)[0], event, ways)

    def go(k, q, level, slot, event, ways):
        if level != "own":
            recv(k, q, slot)
        earlier = before.get((q, level)) if level != "own" else (k - 1 if k else None)
        if ways and earlier is not None:
            done(earlier, q, level, slot, event, ways)
        for copy in sends(k, q, event, slot, ways):
            copy.start()

    def done(k, q, level, slot, event, ways):
        for copy in sends(k, q, event, slot, ways):
            copy.wait_send()

    before = {}

    def step(k, q, level):
        stage(k, q, level, go)
        before[q, level] = k

    def send_own(k, half):
        for q in range(parts):
            if q % 2 == half:

                @pl.when(jnp.logical_and(is_source, q // 2 == core))
                def _(q=q):
                    stage(k, q, "own", go)

    def send_passed(k, half):
        @pl.when(is_source)
        def _():
            passed(k, half, 1 - core).wait_recv()

        for q in range(parts):
            if q % 2 == half:

                @pl.when(jnp.logical_and(is_source, q // 2 != core))
                def _(q=q):
                    stage(k, q, "own", go)

    def multiply(k, half):
        @pl.loop(0, parts // 2)
        def _(i):
            q = 2 * i + half
            left = permuted[k, pl.ds(0, 8), :, lanes(q)].reshape(8 * rows, part)
            product = jnp.dot(
                left, dose[pl.ds(aligned(q * part, 16), part), :], preferred_element_type=jnp.float32
            )
            tiles = [left[:, 128 * t : 128 * (t + 1)].astype(jnp.float32) for t in range(part // 128)]
            while len(tiles) > 1:
                tiles = [sum(tiles[t : t + 2]) for t in range(0, len(tiles), 2)]
            if half:
                score[k] += product
                row_sum[...] += tiles[0]
            else:

                @pl.when(i == 0)
                def _():
                    score[k] = product
                    row_sum[...] = tiles[0]

                @pl.when(i > 0)
                def _():
                    score[k] += product
                    row_sum[...] += tiles[0]

    def center(k, mean_dose):
        sums = jnp.sum(row_sum[...], axis=1, keepdims=True)
        value = score[k] - sums * mean_dose
        score[k] = value
        leaving[k] = value.astype(jnp.bfloat16)

    def score_copies(k):
        copies = []
        for d in (1, 3, 2):
            to = lax.rem(z + d, side)
            copies.append(
                remote(
                    leaving.at[k, pl.ds(aligned(to * 2 * rows, 2 * rows), 2 * rows)],
                    arrived.at[k, d - 1], score_send.at[d - 1], score_recv.at[k, d - 1],
                    to_samp=to * 2 + core,
                )
            )
        return copies

    def inverse_divisor():
        for copy in stat_copies:
            copy.wait_recv()
        sums = jnp.sum(stats[...], axis=0)
        allele_sum, allele_sq = sums[0:1], sums[1:2]
        allele_var = allele_sq / all_samples - (allele_sum / all_samples) ** 2
        inverse = 1.0 / jnp.sqrt(all_samples * (pheno_var + epsilon) * (allele_var + epsilon))
        return inverse, allele_sum / all_samples

    lane = lax.broadcasted_iota(jnp.int32, (2 * rows, 128), 1)

    def local_ends():
        ends = jnp.broadcast_to(marks[...], (8, 128))
        lane8 = lax.broadcasted_iota(jnp.int32, (8, 128), 1)
        offset = 1
        while offset < 128:
            ends = ends + jnp.where(lane8 >= offset, pltpu.roll(ends, offset, axis=1), 0)
            offset *= 2
        return ends - 1 - var * width

    def finish(k, inverse, shared, ends):
        for copy in score_copies(k):
            copy.wait_recv()
        total = score[k, pl.ds(aligned(z * 2 * rows, 2 * rows), 2 * rows), :]
        for d in range(3):
            total = total + arrived[k, d].astype(jnp.float32)
        result = (total + shared) * inverse
        zscore_ref[pl.ds(rows * k, rows), :] = result[:rows]
        zscore_ref[pl.ds(64 + rows * k, rows), :] = result[rows:]
        size = jnp.abs(result)
        best_here = jnp.zeros((2 * rows, 128), jnp.float32)
        for t in range(width // 128):
            run = size[:, 128 * t : 128 * (t + 1)]
            offset = 1
            while offset < 128:
                run = jnp.maximum(run, jnp.where(lane >= offset, pltpu.roll(run, offset, axis=1), 0.0))
                offset *= 2
            here = ends - 128 * t
            source = jnp.minimum(jnp.maximum(here, 0), 127)
            found = jnp.concatenate(
                [
                    jnp.where(
                        here >= 0,
                        jnp.take_along_axis(run[8 * g : 8 * g + 8], source, axis=1, mode="promise_in_bounds"),
                        0.0,
                    )
                    for g in range(2 * rows // 8)
                ],
                axis=0,
            )
            best_here = jnp.maximum(best_here, found)
        best[k] = best_here.astype(jnp.bfloat16)

    def best_copies(k, axis):
        source, target = (best, best_x) if axis == 0 else (best_xy, best_y)
        send, recv_sem = (x_send, x_recv) if axis == 0 else (y_send, y_recv)
        return [
            remote(source.at[k], target.at[k, d - 1], send.at[d - 1], recv_sem.at[k, d - 1], to_var=moved(axis, d))
            for d in (1, 3, 2)
        ]

    def join_x(k):
        for copy in best_copies(k, 0):
            copy.wait_recv()
        value = best[k]
        for d in range(3):
            value = jnp.maximum(value, best_x[k, d])
        best_xy[k] = value

    def join_y(k):
        for copy in best_copies(k, 1):
            copy.wait_recv()
        value = best_xy[k]
        for d in range(3):
            value = jnp.maximum(value, best_y[k, d])
        value = value.astype(jnp.float32)
        thresholds_ref[pl.ds(rows * k, rows), :] = value[:rows]
        thresholds_ref[pl.ds(64 + rows * k, rows), :] = value[rows:]

    def sent_all(copies):
        for copy in copies:
            copy.wait_send()

    def send_best(k, axis):
        if k:
            sent_all(best_copies(k - 1, axis))
        start(best_copies(k, axis))

    def start(copies):
        for copy in copies:
            copy.start()

    def wait_dose():
        dose_copy(1 - core).wait_recv()

    def drain_passed(k):
        @pl.when(jnp.logical_not(is_source))
        def _():
            for half in range(2):
                passed(k, half, core).wait_send()

    last = chunks - 1
    sent, finished, started = False, [], []
    last_send = [e for e in order if e[0] in ("ring", "far", "side", "corner")][-1]
    for name, *where in order:
        if name == "gather":
            gather(*where)
            if where[0] == 0:
                sent_all(trait_copies)
                start([dose_copy(core)] + stat_copies)
            if where[0] == 3:
                read_seg.wait()
                ends = local_ends()
        elif name == "own":
            pass_on(*where)
            send_own(*where)
        elif name == "passed":
            send_passed(*where)
        elif name == "end":
            k, half = where
            for q in range(half, parts, 2):
                stage(k, q, "end", go)
        elif name == "multiply":
            k, half = where
            if k == 0 and half == 0:
                wait_dose()
                inverse, mean_dose = inverse_divisor()
                shared = held_sum * mean_dose
            multiply(k, half)
            if half:
                center(k, mean_dose)
                if k:
                    sent_all(score_copies(k - 1))
                start(score_copies(k))
        elif name == "finish":
            finish(*where, inverse, shared, ends)
            finished.extend(where)
        else:
            step(*where, name)
        if (name, *where) == last_send:
            sent = True
        while sent and len(started) < len(finished):
            started.append(finished[len(started)])
            send_best(started[-1], 0)
    for k in range(last - 1):
        join_x(k)
        send_best(k, 1)
    finish(last, inverse, shared, ends)
    keep_zscore = pltpu.make_async_copy(zscore_ref, zscore_out, local_sem.at[0])
    keep_zscore.start()
    send_best(last, 0)
    join_x(last - 1)
    send_best(last - 1, 1)
    sent_all(stat_copies + [dose_copy(core)])
    drain_passed(last)
    for q in range(parts):
        stage(last, q, "own", done)
        for level in ("ring", "far", "side", "corner"):
            stage(before[q, level], q, level, done)
    sent_all(score_copies(last))
    for k in range(last - 1):
        join_y(k)
    join_x(last)
    send_best(last, 1)
    join_y(last - 1)
    sent_all(best_copies(last, 0))
    join_y(last)
    keep = pltpu.make_async_copy(thresholds_ref, thresholds_out, local_sem.at[1])
    keep.start()
    sent_all(best_copies(last, 1))
    keep_zscore.wait()
    keep.wait()


def keep_kernel(zscore_ref, thresholds_ref, zscore_out, thresholds_out, first, second, sem):
    into = [
        pltpu.make_async_copy(zscore_ref, first, sem.at[0]),
        pltpu.make_async_copy(thresholds_ref, second, sem.at[1]),
    ]
    out = [
        pltpu.make_async_copy(first, zscore_out, sem.at[2]),
        pltpu.make_async_copy(second, thresholds_out, sem.at[3]),
    ]
    for copy in into:
        copy.start()
    for copy, after in zip(into, out):
        copy.wait()
        after.start()
    for copy in out:
        copy.wait()


def per_device(dosage, phenotype, perm_index, seg_lengths):
    samples, width = dosage.shape
    segments = seg_lengths.shape[0]
    dma = pltpu.SemaphoreType.DMA
    f32, i32, bf16 = jnp.float32, jnp.int32, jnp.bfloat16
    vmem = pltpu.VMEM
    any_space = pl.BlockSpec(memory_space=pltpu.HBM)
    outs = (
        jax.ShapeDtypeStruct((128, width), f32),
        jax.ShapeDtypeStruct((128, segments), f32),
    )
    zscore, thresholds = pl.pallas_call(
        kernel,
        out_shape=outs,
        in_specs=[any_space] * 4,
        out_specs=(any_space, any_space),
        scratch_shapes=[
            vmem((128, width), f32),
            vmem((128, segments), f32),
            vmem((8, samples // 128, 128), f32),
            vmem((samples * 4 // 128, 128), i32),
            vmem((samples * 4 // 16, 128), i32),
            vmem(perm_index.shape, i32),
            vmem((samples, width), i32),
            vmem((2 * samples, width), bf16),
            vmem((chunks, 9, rows, 2 * samples), bf16),
            vmem((chunks, 8 * rows, width), f32),
            vmem((8 * rows, 128), f32),
            vmem((chunks, 8 * rows, width), bf16),
            vmem((chunks, 3, 2 * rows, width), bf16),
            vmem((8, 8, width), f32),
            vmem((1, segments), i32),
            vmem((chunks, 2 * rows, segments), bf16),
            vmem((chunks, 3, 2 * rows, segments), bf16),
            vmem((chunks, 2 * rows, segments), bf16),
            vmem((chunks, 3, 2 * rows, segments), bf16),
            dma((3 + pieces,)),
            dma((7,)),
            dma((7,)),
            dma((7,)),
            dma((1,)),
            dma((1,)),
            dma((2,)),
            dma((chunks, 2)),
            dma((parts, 15)),
            dma((chunks, parts, 8)),
            dma((3,)),
            dma((chunks, 3)),
            dma((3,)),
            dma((chunks, 3)),
            dma((3,)),
            dma((chunks, 3)),
        ],
        compiler_params=pltpu.CompilerParams(
            collective_id=0, has_side_effects=True, vmem_limit_bytes=60 * 1024 * 1024
        ),
    )(
        dosage,
        phenotype.reshape(samples // 128, 128),
        perm_index,
        seg_lengths.reshape(1, segments),
    )
    return pl.pallas_call(
        keep_kernel,
        out_shape=outs,
        in_specs=[any_space] * 2,
        out_specs=(any_space, any_space),
        scratch_shapes=[vmem((128, width), f32), vmem((128, segments), f32), dma((4,))],
        compiler_params=pltpu.CompilerParams(vmem_limit_bytes=60 * 1024 * 1024),
    )(zscore, thresholds)


def solution(mesh):
    return jax.shard_map(
        per_device,
        mesh=mesh,
        in_specs=(P("samp", "var"), P("samp"), P("var", "samp"), P()),
        out_specs=(P("samp", "var"), P("samp", None)),
        check_vma=False,
    )
```
